64 devices in a mesh: prob: 4 (over x, y), feat: 16 (over z, core).
Axes of the slice: x: 2, y: 2, z: 8, core: 2. Of those that a mesh axis runs over, the one named last changes fastest.
The devices are a block of a 4x4x8 slice.
Arguments:
- design: bfloat16 [16384, 32768], P('prob', 'feat'), parts along dimension 0
- targets: float32 [16384, 300], P('prob'), parts along dimension 0
- weights_init: float32 [131072, 300], P(('prob', 'feat')), parts along dimension 0
- step_sizes: float32 [131072], P(('prob', 'feat')), parts along dimension 0
Outputs:
- output 1: float32 [131072, 300], P(('prob', 'feat')), parts along dimension 0
- output 2: float32 [16384, 300], P('prob'), parts along dimension 0
There are 4 independent parts. The reference program is written for one: setup_inputs(seed, part) draws one part's arguments, and reference() takes and returns one part's arrays. A program takes and returns all parts, laid end to end along the dimension named above; each array names one.
All inputs are finite; a program needn't handle non-finite values.
Results may differ from the reference program's by a relative error of at most 0.001.
Values are sent between devices in bfloat16 or wider.
A program may use at most 768 MiB of HBM per device.

```python
import jax
import jax.numpy as jnp
from jax import lax

SAMPLES = 4096
TARGETS = 300
FEATURES = 32768
SWEEPS = 6
SPIKE_RANK = 4
RIDGE_COEF = 1.0
MIX_WEIGHT = 0.75
STEP_TOTAL = 2.0


def spectral_bound(design, step_gain, rng_key):
    ridge_val = RIDGE_COEF / SAMPLES

    def apply_op(probe_vec):
        proj_rows = jnp.dot(design, probe_vec.astype(jnp.bfloat16), preferred_element_type=jnp.float32)
        back_cols = jnp.dot(proj_rows.astype(jnp.bfloat16), design, preferred_element_type=jnp.float32)
        return step_gain * (back_cols / SAMPLES + ridge_val * probe_vec)

    def power_step(step_idx, probe_vec):
        image_vec = apply_op(probe_vec)
        return image_vec / jnp.linalg.norm(image_vec)

    start_vec = jax.random.normal(rng_key, (FEATURES,), jnp.float32)
    probe_vec = lax.fori_loop(0, 24, power_step, start_vec / jnp.linalg.norm(start_vec))
    return jnp.linalg.norm(apply_op(probe_vec))


def setup_inputs(seed: int = 0, part: int = 0) -> dict:
    sub_keys = jax.random.split(jax.random.fold_in(jax.random.key(seed), part), 8)
    bulk_edge = (SAMPLES ** -0.5 + FEATURES ** -0.5) ** 2
    spike_amp = (2.0 * bulk_edge) ** 0.5
    noise_mat = jax.random.normal(sub_keys[0], (SAMPLES, FEATURES), jnp.float32)
    factors = jax.random.normal(sub_keys[1], (SAMPLES, SPIKE_RANK), jnp.float32)
    loadings = jax.random.normal(sub_keys[2], (SPIKE_RANK, FEATURES), jnp.float32)
    dense_x = (noise_mat + spike_amp * jnp.dot(factors, loadings)) * FEATURES ** -0.5
    design = dense_x.astype(jnp.bfloat16)
    coef_true = jax.random.normal(sub_keys[3], (FEATURES, TARGETS), jnp.float32)
    targets = jnp.dot(dense_x, coef_true) + 0.5 * jax.random.normal(sub_keys[4], (SAMPLES, TARGETS), jnp.float32)
    weights_init = jax.random.normal(sub_keys[5], (FEATURES, TARGETS), jnp.float32)
    step_gain = jax.random.uniform(sub_keys[6], (FEATURES,), jnp.float32, 0.25, 1.75)
    top_eig = spectral_bound(design, step_gain, sub_keys[7])
    step_sizes = step_gain * (STEP_TOTAL / SWEEPS) / (1.15 * top_eig)
    return {'design': design, 'targets': targets, 'weights_init': weights_init, 'step_sizes': step_sizes}


def reference(design, targets, weights_init, step_sizes):
    ridge_val = RIDGE_COEF / SAMPLES
    step_col = step_sizes[:, None]
    residual = targets - jnp.dot(design, weights_init.astype(jnp.bfloat16), preferred_element_type=jnp.float32)

    def one_sweep(state_pair, unused):
        weights, residual = state_pair
        gradient = lax.dot_general(design, residual.astype(jnp.bfloat16), (((0,), (0,)), ((), ())), preferred_element_type=jnp.float32) / SAMPLES
        update = step_col * (gradient - ridge_val * weights)
        weights = weights + MIX_WEIGHT * update
        residual = residual - MIX_WEIGHT * jnp.dot(design, update.astype(jnp.bfloat16), preferred_element_type=jnp.float32)
        return (weights, residual), None

    (weights, residual), unused_out = lax.scan(one_sweep, (weights_init, residual), None, length=SWEEPS)
    return weights, residual
```

```python
import functools

import jax
import jax.numpy as jnp
from jax import lax
from jax.experimental import pallas as pl
from jax.experimental.pallas import tpu as pltpu
from jax.sharding import PartitionSpec as P

SWEEPS = 6
RIDGE_COEF = 1.0
MIX_WEIGHT = 0.75
CORES = 2
ROW_TILE = 16
MESH = pl.DeviceIdType.MESH


def split_rows(padded):
    first = -(-padded // (2 * ROW_TILE)) * ROW_TILE
    return ((0, first), (first, padded - first))


def kernel(chips, samples, streams, x_hbm, w_hbm, y_hbm, eta_ref, wout_hbm, rout_hbm,
           x, w, res, grad, op, xsem, wsem, ysem, wosem, *rest):
    per = len(rest) // len(streams)
    st = [rest[i * per:(i + 1) * per] for i in range(len(streams))]
    far, near = chips // 2, chips - 1 - chips // 2
    block = samples // (chips * CORES)
    rows_chip = block * CORES
    depth = x.shape[1]
    ridge_val = RIDGE_COEF / samples

    prob = lax.axis_index("prob")
    feat = lax.axis_index("feat")
    z, c = feat // CORES, feat % CORES
    other = 1 - c
    sgn = 1 - 2 * c

    def chip_at(v):
        return lax.rem(z + v * sgn + chips, chips)

    sib = (prob, z * CORES + other)
    nbr_p = (prob, chip_at(1) * CORES + c)
    nbr_q = (prob, chip_at(-1) * CORES + c)

    def x_rows(v):
        return pl.ds(pl.multiple_of(chip_at(v) * rows_chip, rows_chip), rows_chip)

    def remote(src, dst, ssem, rsem, dev):
        return pltpu.make_async_remote_copy(src_ref=src, dst_ref=dst, send_sem=ssem, recv_sem=rsem,
                                            device_id=dev, device_id_type=MESH)

    def x_copy(v):
        return pltpu.make_async_copy(x_hbm.at[x_rows(v), :], x.at[x_rows(v), :], xsem.at[v % chips])

    class Stream:
        def __init__(self, index):
            self.r0, self.rows = streams[index]
            self.rs = pl.ds(self.r0, self.rows)
            (self.pbuf, self.precv, self.rp, self.rq, self.rbf, self.rfin,
             self.pd_s, self.pd_r, self.rsp_s, self.rsp_r, self.rsq_s, self.rsq_r,
             self.agp_s, self.agp_r, self.agq_s, self.agq_r, self.agd_s, self.agd_r, self.osem) = st[index]

        def pd(self, v):
            a, b = v % chips, -v % chips
            return remote(self.pbuf.at[a, other], self.precv.at[b], self.pd_s.at[a], self.pd_r.at[b], sib)

        def rs_p(self, t):
            return remote(self.pbuf.at[far + 1 - t, c], self.rp.at[t - 1], self.rsp_s.at[t - 1],
                          self.rsp_r.at[t - 1], nbr_p)

        def rs_q(self, t):
            return remote(self.pbuf.at[-(near + 1 - t) % chips, c], self.rq.at[t - 1], self.rsq_s.at[t - 1],
                          self.rsq_r.at[t - 1], nbr_q)

        def ag_p(self, buf, t):
            return remote(buf.at[t - 1, c], buf.at[t, c], self.agp_s.at[t - 1], self.agp_r.at[t - 1], nbr_p)

        def ag_q(self, buf, t):
            return remote(buf.at[-(t - 1) % chips, c], buf.at[-t % chips, c], self.agq_s.at[t - 1],
                          self.agq_r.at[t - 1], nbr_q)

        def ag_d(self, buf, u):
            a, b = u % chips, -u % chips
            return remote(buf.at[a, c], buf.at[b, c], self.agd_s.at[a], self.agd_r.at[b], sib)

        def ag_d_in(self, buf, u):
            a = u % chips
            return remote(buf.at[a, other], buf.at[a, other], self.agd_s.at[a], self.agd_r.at[a], sib)

        def product(self, v):
            out = lax.dot_general(op[self.rs, :], x[x_rows(v), :], (((1,), (1,)), ((), ())),
                                  preferred_element_type=jnp.float32)
            for core in range(CORES):
                self.pbuf[v % chips, core] = out[:, core * block:(core + 1) * block]
            self.pd(v).start()

        def pass_on(self, t):
            v = far + 1 - t
            self.pd(-v).wait_recv()
            total = self.pbuf[v, c] + self.precv[v]
            if t > 1:
                self.rs_p(t - 1).wait_recv()
                total = total + self.rp[t - 2]
            self.pbuf[v, c] = total
            self.rs_p(t).start()
            t = t - 1
            if t >= 1:
                v = near + 1 - t
                slot = -v % chips
                self.pd(v).wait_recv()
                total = self.pbuf[slot, c] + self.precv[slot]
                if t > 1:
                    self.rs_q(t - 1).wait_recv()
                    total = total + self.rq[t - 2]
                self.pbuf[slot, c] = total
                self.rs_q(t).start()

        def finish(self, it):
            self.pd(0).wait_recv()
            total = self.pbuf[0, c] + self.precv[0]
            self.rs_p(far).wait_recv()
            self.rs_q(near).wait_recv()
            total = total + self.rp[far - 1] + self.rq[near - 1]
            coef = jnp.where(it == 0, 1.0, MIX_WEIGHT).astype(jnp.float32)
            new = res[self.rs, :] - coef * total
            res[self.rs, :] = new

            @pl.when(it < SWEEPS)
            def _():
                self.rbf[0, c] = new.astype(jnp.bfloat16)
                self.ag_open(self.rbf)

            @pl.when(it == SWEEPS)
            def _():
                self.rfin[0, c] = new
                self.ag_open(self.rfin)

        def ag_open(self, buf):
            self.ag_p(buf, 1).start()
            self.ag_q(buf, 1).start()
            self.ag_d(buf, 0).start()

        def ag_step(self, buf, t):
            self.ag_p(buf, t).wait_recv()
            if t < far:
                self.ag_p(buf, t + 1).start()
            if t <= near:
                self.ag_q(buf, t).wait_recv()
                if t < near:
                    self.ag_q(buf, t + 1).start()
            self.ag_d(buf, t).start()
            if t <= near:
                self.ag_d(buf, -t).start()

        def settle_sums(self):
            for v in range(chips):
                self.pd(v).wait_send()
            for t in range(1, far + 1):
                self.rs_p(t).wait_send()
            for t in range(1, near + 1):
                self.rs_q(t).wait_send()

        def settle_gather(self, buf):
            for t in range(1, far + 1):
                self.ag_p(buf, t).wait_send()
            for t in range(1, near + 1):
                self.ag_q(buf, t).wait_send()
            for u in range(chips):
                self.ag_d(buf, u).wait_send()

        def gradient(self, t):
            offsets = (t, -t) if 0 < t <= near else (t,)
            parts = []
            for u in offsets:
                self.ag_d_in(self.rbf, u).wait_recv()
                parts.append((jnp.concatenate([self.rbf[u % chips, core] for core in range(CORES)], axis=1), x_rows(-u)))
            wide = min(depth, 1024)
            for j in range(depth // wide):
                cols = pl.ds(j * wide, wide)
                total = None if t == 0 else grad[self.rs, cols]
                for lhs, where in parts:
                    term = jnp.dot(lhs, x[where, cols], preferred_element_type=jnp.float32)
                    total = term if total is None else total + term
                grad[self.rs, cols] = total

        def step(self):
            @pl.loop(0, self.rows // ROW_TILE)
            def _(i):
                rs = pl.ds(pl.multiple_of(self.r0 + i * ROW_TILE, ROW_TILE), ROW_TILE)
                old = w[rs, :]
                update = eta_ref[...] * (grad[rs, :] * (1.0 / samples) - ridge_val * old)
                w[rs, :] = old + MIX_WEIGHT * update
                op[rs, :] = update.astype(jnp.bfloat16)

        def cast(self):
            @pl.loop(0, self.rows // ROW_TILE)
            def _(i):
                rs = pl.ds(pl.multiple_of(self.r0 + i * ROW_TILE, ROW_TILE), ROW_TILE)
                op[rs, :] = w[rs, :].astype(jnp.bfloat16)

        def write(self, u, core):
            return pltpu.make_async_copy(self.rfin.at[u % chips, core],
                                         rout_hbm.at[chip_at(-u) * CORES + core, self.rs, :],
                                         self.osem.at[u % chips, core])

    group = [Stream(i) for i in range(len(streams))]
    order = [far] + [s * v for v in range(near, 0, -1) for s in (1, -1)] + [0]

    w_copy = pltpu.make_async_copy(w_hbm, w, wsem)
    w_copy.start()
    x_copy(far).start()
    for v in order[1:]:
        x_copy(v).start()
    y_copy = pltpu.make_async_copy(y_hbm, res, ysem)
    y_copy.start()

    barrier = pltpu.get_barrier_semaphore()
    for dev in (sib, nbr_p, nbr_q):
        pl.semaphore_signal(barrier, inc=1, device_id=dev, device_id_type=MESH)
    pl.semaphore_wait(barrier, 3)

    w_copy.wait()
    for s in group:
        s.cast()
    x_copy(far).wait()
    for s in group:
        s.product(far)
    y_copy.wait()

    @pl.loop(0, SWEEPS + 1)
    def _(it):
        def products(s, vs):
            for v in vs:
                if s is group[0]:
                    @pl.when(it == 0)
                    def _():
                        x_copy(v).wait()
                s.product(v)

        for t in range(1, far + 1):
            v = far - t
            vs = (v, -v) if v else (0,)
            for s in group:
                s.pass_on(t)
                products(s, vs)
        for s in group:
            s.finish(it)
        for s in group:
            s.settle_sums()

        @pl.when(it < SWEEPS)
        def _():
            for t in range(1, far + 1):
                for s in group:
                    s.ag_step(s.rbf, t)
                    s.gradient(t - 1)
            for s in group:
                s.gradient(far)
                s.step()
                s.settle_gather(s.rbf)
                s.product(far)

    w_out = pltpu.make_async_copy(w, wout_hbm, wosem)
    w_out.start()
    for s in group:
        s.write(0, c).start()
    for t in range(1, far + 1):
        for s in group:
            s.ag_step(s.rfin, t)
            s.write(t, c).start()
            if t <= near:
                s.write(-t, c).start()
            us = (0,) if t == 1 else (t - 1, 1 - t)
            for u in us:
                s.ag_d_in(s.rfin, u).wait_recv()
                s.write(u, other).start()
    for s in group:
        s.ag_d_in(s.rfin, far).wait_recv()
        s.write(far, other).start()
    for s in group:
        s.settle_gather(s.rfin)
        for u in range(chips):
            for core in (c, other):
                s.write(u, core).wait()
    w_out.wait()


def solve(chips, design, w_t, y_t, eta):
    samples, depth = design.shape
    padded = w_t.shape[0]
    block = y_t.shape[1]
    far, near = chips // 2, chips - 1 - chips // 2
    streams = split_rows(padded)
    dma = pltpu.SemaphoreType.DMA
    f32, bf16 = jnp.float32, jnp.bfloat16
    scratch = [
        pltpu.VMEM((samples, depth), bf16),
        pltpu.VMEM((padded, depth), f32),
        pltpu.VMEM((padded, block), f32),
        pltpu.VMEM((padded, depth), f32),
        pltpu.VMEM((padded, depth), bf16),
        dma((chips,)), dma, dma, dma,
    ]
    for _, rows in streams:
        scratch += [
            pltpu.VMEM((chips, CORES, rows, block), f32),
            pltpu.VMEM((chips, rows, block), f32),
            pltpu.VMEM((far, rows, block), f32),
            pltpu.VMEM((near, rows, block), f32),
            pltpu.VMEM((chips, CORES, rows, block), bf16),
            pltpu.VMEM((chips, CORES, rows, block), f32),
            dma((chips,)), dma((chips,)),
            dma((far,)), dma((far,)), dma((near,)), dma((near,)),
            dma((far,)), dma((far,)), dma((near,)), dma((near,)),
            dma((chips,)), dma((chips,)),
            dma((chips, CORES)),
        ]
    any_spec = pl.BlockSpec(memory_space=pl.ANY)
    return pl.pallas_call(
        functools.partial(kernel, chips, samples, streams),
        out_shape=(jax.ShapeDtypeStruct((padded, depth), f32),
                   jax.ShapeDtypeStruct((chips * CORES, padded, block), f32)),
        in_specs=[any_spec, any_spec, any_spec, pl.BlockSpec(memory_space=pltpu.VMEM)],
        out_specs=(any_spec, any_spec),
        scratch_shapes=scratch,
        compiler_params=pltpu.CompilerParams(collective_id=0, has_side_effects=True,
                                             vmem_limit_bytes=56 * 1024 * 1024),
    )(design, w_t, y_t, eta)


def solution(mesh):
    feats = mesh.shape["feat"]

    def local_solve(design, targets, weights, step_sizes):
        samples, depth = design.shape
        k = targets.shape[1]
        padded = -(-k // ROW_TILE) * ROW_TILE
        block = samples // feats
        pad = ((0, padded - k), (0, 0))
        w_t = jnp.pad(weights.T, pad)
        mine = lax.dynamic_slice_in_dim(targets, lax.axis_index("feat") * block, block, 0)
        y_t = jnp.pad(mine.T, pad)
        w_new, r_new = solve(feats // CORES, design, w_t, y_t, step_sizes[None, :])
        residual = r_new[:, :k, :].transpose(0, 2, 1).reshape(samples, k)
        return w_new[:k].T, residual

    return jax.shard_map(
        local_solve,
        mesh=mesh,
        in_specs=(P('prob', 'feat'), P('prob', None), P(('prob', 'feat'), None), P(('prob', 'feat'))),
        out_specs=(P(('prob', 'feat'), None), P('prob', None)),
        check_vma=False,
    )
```

```python
import functools

import jax
import jax.numpy as jnp
from jax import lax
from jax.experimental import pallas as pl
from jax.experimental.pallas import tpu as pltpu
from jax.sharding import PartitionSpec as P

SWEEPS = 6
RIDGE_COEF = 1.0
MIX_WEIGHT = 0.75
CORES = 2
ROW_TILE = 16
PIECES = 2
MESH = pl.DeviceIdType.MESH


def split_rows(padded):
    first = -(-padded // (2 * ROW_TILE)) * ROW_TILE
    return ((0, first), (first, padded - first))


def split_pieces(rows):
    size = -(-rows // (PIECES * ROW_TILE)) * ROW_TILE
    return tuple((r, min(size, rows - r)) for r in range(0, rows, size))


def kernel(chips, samples, streams, x_hbm, w_hbm, y_hbm, eta_ref, wout_hbm, rout_hbm,
           x, wraw, yraw, w, res, grad, op, xsem, wsem, ysem, wosem, *rest):
    per = len(rest) // len(streams)
    st = [rest[i * per:(i + 1) * per] for i in range(len(streams))]
    far, near = chips // 2, chips - 1 - chips // 2
    block = samples // (chips * CORES)
    rows_chip = block * CORES
    depth = x.shape[1]
    ridge_val = RIDGE_COEF / samples

    prob = lax.axis_index("prob")
    feat = lax.axis_index("feat")
    z, c = feat // CORES, feat % CORES
    other = 1 - c
    sgn = 1 - 2 * c

    def chip_at(v):
        return lax.rem(z + v * sgn + chips, chips)

    sib = (prob, z * CORES + other)
    nbr_p = (prob, chip_at(1) * CORES + c)
    nbr_q = (prob, chip_at(-1) * CORES + c)

    def x_rows(v):
        return pl.ds(pl.multiple_of(chip_at(v) * rows_chip, rows_chip), rows_chip)

    def remote(src, dst, ssem, rsem, dev):
        return pltpu.make_async_remote_copy(src_ref=src, dst_ref=dst, send_sem=ssem, recv_sem=rsem,
                                            device_id=dev, device_id_type=MESH)

    def x_copy(v):
        return pltpu.make_async_copy(x_hbm.at[x_rows(v), :], x.at[x_rows(v), :], xsem.at[v % chips])

    class Stream:
        def __init__(self, index):
            self.r0, self.rows = streams[index]
            self.rs = pl.ds(self.r0, self.rows)
            self.cuts = split_pieces(self.rows)
            self.pieces = range(len(self.cuts))
            (self.pbuf, self.precv, self.rp, self.rq, self.rbf, self.rfin,
             self.pd_s, self.pd_r, self.rsp_s, self.rsp_r, self.rsq_s, self.rsq_r,
             self.agp_s, self.agp_r, self.agq_s, self.agq_r, self.agd_s, self.agd_r, self.osem) = st[index]

        def ps(self, p):
            return pl.ds(*self.cuts[p])

        def pd(self, v):
            a, b = v % chips, -v % chips
            return remote(self.pbuf.at[a, other], self.precv.at[b], self.pd_s.at[a], self.pd_r.at[b], sib)

        def rs_p(self, t, p):
            ps = self.ps(p)
            return remote(self.pbuf.at[far + 1 - t, c, ps], self.rp.at[t - 1, ps], self.rsp_s.at[t - 1, p],
                          self.rsp_r.at[t - 1, p], nbr_p)

        def rs_q(self, t, p):
            ps = self.ps(p)
            return remote(self.pbuf.at[-(near + 1 - t) % chips, c, ps], self.rq.at[t - 1, ps],
                          self.rsq_s.at[t - 1, p], self.rsq_r.at[t - 1, p], nbr_q)

        def ag_p(self, buf, t, p):
            ps = self.ps(p)
            return remote(buf.at[t - 1, c, ps], buf.at[t, c, ps], self.agp_s.at[t - 1, p],
                          self.agp_r.at[t - 1, p], nbr_p)

        def ag_q(self, buf, t, p):
            ps = self.ps(p)
            return remote(buf.at[-(t - 1) % chips, c, ps], buf.at[-t % chips, c, ps], self.agq_s.at[t - 1, p],
                          self.agq_r.at[t - 1, p], nbr_q)

        def ag_d(self, buf, u, p):
            a, b, ps = u % chips, -u % chips, self.ps(p)
            return remote(buf.at[a, c, ps], buf.at[b, c, ps], self.agd_s.at[a, p], self.agd_r.at[b, p], sib)

        def ag_d_in(self, buf, u, p):
            a, ps = u % chips, self.ps(p)
            return remote(buf.at[a, other, ps], buf.at[a, other, ps], self.agd_s.at[a, p], self.agd_r.at[a, p], sib)

        def product(self, v):
            out = lax.dot_general(op[self.rs, :], x[x_rows(v), :], (((1,), (1,)), ((), ())),
                                  preferred_element_type=jnp.float32)
            for core in range(CORES):
                self.pbuf[v % chips, core] = out[:, core * block:(core + 1) * block]
            self.pd(v).start()

        def pass_on(self, t, p):
            ps = self.ps(p)
            v = far + 1 - t
            if p == 0:
                self.pd(-v).wait_recv()
            total = self.pbuf[v, c, ps] + self.precv[v, ps]
            if t > 1:
                self.rs_p(t - 1, p).wait_recv()
                total = total + self.rp[t - 2, ps]
            self.pbuf[v, c, ps] = total
            self.rs_p(t, p).start()
            t = t - 1
            if t >= 1:
                v = near + 1 - t
                slot = -v % chips
                if p == 0:
                    self.pd(v).wait_recv()
                total = self.pbuf[slot, c, ps] + self.precv[slot, ps]
                if t > 1:
                    self.rs_q(t - 1, p).wait_recv()
                    total = total + self.rq[t - 2, ps]
                self.pbuf[slot, c, ps] = total
                self.rs_q(t, p).start()

        def finish(self, it, p):
            ps = self.ps(p)
            if p == 0:
                self.pd(0).wait_recv()
            total = self.pbuf[0, c, ps] + self.precv[0, ps]
            self.rs_p(far, p).wait_recv()
            self.rs_q(near, p).wait_recv()
            total = total + self.rp[far - 1, ps] + self.rq[near - 1, ps]
            coef = jnp.where(it == 0, 1.0, MIX_WEIGHT).astype(jnp.float32)
            start, size = self.cuts[p]
            rs = pl.ds(self.r0 + start, size)
            new = res[rs, :] - coef * total
            res[rs, :] = new

            @pl.when(it < SWEEPS)
            def _():
                self.rbf[0, c, ps] = new.astype(jnp.bfloat16)
                self.ag_open(self.rbf, p)

            @pl.when(it == SWEEPS)
            def _():
                self.rfin[0, c, ps] = new
                self.ag_open(self.rfin, p)

        def ag_open(self, buf, p):
            self.ag_p(buf, 1, p).start()
            self.ag_q(buf, 1, p).start()
            self.ag_d(buf, 0, p).start()

        def ag_step(self, buf, t, p):
            self.ag_p(buf, t, p).wait_recv()
            if t < far:
                self.ag_p(buf, t + 1, p).start()
            self.ag_d(buf, t, p).start()
            if t <= near:
                self.ag_q(buf, t, p).wait_recv()
                if t < near:
                    self.ag_q(buf, t + 1, p).start()
                self.ag_d(buf, -t, p).start()

        def settle_sums(self):
            for v in range(chips):
                self.pd(v).wait_send()
            for p in self.pieces:
                for t in range(1, far + 1):
                    self.rs_p(t, p).wait_send()
                for t in range(1, near + 1):
                    self.rs_q(t, p).wait_send()

        def settle_gather(self, buf):
            for p in self.pieces:
                for t in range(1, far + 1):
                    self.ag_p(buf, t, p).wait_send()
                for t in range(1, near + 1):
                    self.ag_q(buf, t, p).wait_send()
                for u in range(chips):
                    self.ag_d(buf, u, p).wait_send()

        def gradient(self, t):
            offsets = (t, -t) if 0 < t <= near else (t,)
            parts = []
            for u in offsets:
                for p in self.pieces:
                    self.ag_d_in(self.rbf, u, p).wait_recv()
                parts.append((jnp.concatenate([self.rbf[u % chips, core] for core in range(CORES)], axis=1), x_rows(-u)))
            wide = min(depth, 1024)
            for j in range(depth // wide):
                cols = pl.ds(j * wide, wide)
                total = None if t == 0 else grad[self.rs, cols]
                for lhs, where in parts:
                    term = jnp.dot(lhs, x[where, cols], preferred_element_type=jnp.float32)
                    total = term if total is None else total + term
                grad[self.rs, cols] = total

        def step(self):
            @pl.loop(0, self.rows // ROW_TILE)
            def _(i):
                rs = pl.ds(pl.multiple_of(self.r0 + i * ROW_TILE, ROW_TILE), ROW_TILE)
                old = w[rs, :]
                update = eta_ref[...] * (grad[rs, :] * (1.0 / samples) - ridge_val * old)
                w[rs, :] = old + MIX_WEIGHT * update
                op[rs, :] = update.astype(jnp.bfloat16)

        def cast(self):
            k = wraw.shape[0]
            real = min(self.rows, k - self.r0)

            def move(rs):
                rows = wraw[rs, :]
                w[rs, :] = rows
                op[rs, :] = rows.astype(jnp.bfloat16)

            @pl.loop(0, real // ROW_TILE)
            def _(i):
                move(pl.ds(pl.multiple_of(self.r0 + i * ROW_TILE, ROW_TILE), ROW_TILE))

            if real % ROW_TILE:
                move(pl.ds(self.r0 + real // ROW_TILE * ROW_TILE, real % ROW_TILE))

        def write(self, u, core):
            return pltpu.make_async_copy(self.rfin.at[u % chips, core],
                                         rout_hbm.at[self.rs, pl.ds(pl.multiple_of((chip_at(-u) * CORES + core) * block, block), block)],
                                         self.osem.at[u % chips, core])

    group = [Stream(i) for i in range(len(streams))]
    order = [far] + [s * v for v in range(near, 0, -1) for s in (1, -1)] + [0]

    w_copy = pltpu.make_async_copy(w_hbm, wraw, wsem)
    w_copy.start()
    x_copy(far).start()
    for v in order[1:]:
        x_copy(v).start()
    mine = pl.ds(pl.multiple_of(feat * block, block), block)
    y_copy = pltpu.make_async_copy(y_hbm.at[:, mine], yraw, ysem)
    y_copy.start()

    barrier = pltpu.get_barrier_semaphore()
    for dev in (sib, nbr_p, nbr_q):
        pl.semaphore_signal(barrier, inc=1, device_id=dev, device_id_type=MESH)
    pl.semaphore_wait(barrier, 3)

    w_copy.wait()
    for s in group:
        s.cast()
    x_copy(far).wait()
    for s in group:
        s.product(far)
    y_copy.wait()
    res[pl.ds(0, yraw.shape[0]), :] = yraw[...]

    @pl.loop(0, SWEEPS + 1)
    def _(it):
        def products(s, vs):
            for v in vs:
                if s is group[0]:
                    @pl.when(it == 0)
                    def _():
                        x_copy(v).wait()
                s.product(v)

        for t in range(1, far + 1):
            v = far - t
            vs = (v, -v) if v else (0,)
            for s in group:
                for p in s.pieces:
                    s.pass_on(t, p)
                products(s, vs)
        for s in group:
            for p in s.pieces:
                s.finish(it, p)
        for s in group:
            s.settle_sums()

        @pl.when(it < SWEEPS)
        def _():
            for t in range(1, far + 1):
                for s in group:
                    for p in s.pieces:
                        s.ag_step(s.rbf, t, p)
                    s.gradient(t - 1)
                    if t == far:
                        s.gradient(far)
                        s.step()
                        s.settle_gather(s.rbf)
                        s.product(far)

    w_out = pltpu.make_async_copy(w, wout_hbm, wosem)
    w_out.start()

    def write_in(s, u):
        for p in s.pieces:
            s.ag_d_in(s.rfin, u, p).wait_recv()
        s.write(u, other).start()

    for s in group:
        s.write(0, c).start()
    for t in range(1, far + 1):
        for s in group:
            for p in s.pieces:
                s.ag_step(s.rfin, t, p)
            s.write(t, c).start()
            if t <= near:
                s.write(-t, c).start()
            for u in ((0,) if t == 1 else (t - 1, 1 - t)):
                write_in(s, u)
    for s in group:
        write_in(s, far)
    for s in group:
        s.settle_gather(s.rfin)
        for u in range(chips):
            for core in (c, other):
                s.write(u, core).wait()
    w_out.wait()


def solve(chips, design, w_t, y_t, eta):
    samples, depth = design.shape
    padded = -(-w_t.shape[0] // ROW_TILE) * ROW_TILE
    block = samples // (chips * CORES)
    far, near = chips // 2, chips - 1 - chips // 2
    streams = split_rows(padded)
    dma = pltpu.SemaphoreType.DMA
    f32, bf16 = jnp.float32, jnp.bfloat16
    scratch = [
        pltpu.VMEM((samples, depth), bf16),
        pltpu.VMEM((w_t.shape[0], depth), f32),
        pltpu.VMEM((w_t.shape[0], block), f32),
        pltpu.VMEM((padded, depth), f32),
        pltpu.VMEM((padded, block), f32),
        pltpu.VMEM((padded, depth), f32),
        pltpu.VMEM((padded, depth), bf16),
        dma((chips,)), dma, dma, dma,
    ]
    for _, rows in streams:
        scratch += [
            pltpu.VMEM((chips, CORES, rows, block), f32),
            pltpu.VMEM((chips, rows, block), f32),
            pltpu.VMEM((far, rows, block), f32),
            pltpu.VMEM((near, rows, block), f32),
            pltpu.VMEM((chips, CORES, rows, block), bf16),
            pltpu.VMEM((chips, CORES, rows, block), f32),
            dma((chips,)), dma((chips,)),
            *[dma((hops, PIECES)) for hops in (far, far, near, near) * 2],
            dma((chips, PIECES)), dma((chips, PIECES)),
            dma((chips, CORES)),
        ]
    any_spec = pl.BlockSpec(memory_space=pl.ANY)
    return pl.pallas_call(
        functools.partial(kernel, chips, samples, streams),
        out_shape=(jax.ShapeDtypeStruct((padded, depth), f32),
                   jax.ShapeDtypeStruct((padded, samples), f32)),
        in_specs=[any_spec, any_spec, any_spec, pl.BlockSpec(memory_space=pltpu.VMEM)],
        out_specs=(any_spec, any_spec),
        scratch_shapes=scratch,
        compiler_params=pltpu.CompilerParams(collective_id=0, has_side_effects=True,
                                             vmem_limit_bytes=56 * 1024 * 1024),
    )(design, w_t, y_t, eta)


def trim_kernel(k, w_in, r_in, w_out, r_out):
    w_out[...] = w_in[:k, :]
    r_out[...] = r_in[:k, :]


def trim(k, steps, w_t, r_t):
    def spec(rows, arr):
        return pl.BlockSpec((rows, arr.shape[1] // steps), lambda i: (0, i))

    return pl.pallas_call(
        functools.partial(trim_kernel, k),
        out_shape=tuple(jax.ShapeDtypeStruct((k, a.shape[1]), a.dtype) for a in (w_t, r_t)),
        grid=(steps,),
        in_specs=[spec(a.shape[0], a) for a in (w_t, r_t)],
        out_specs=tuple(spec(k, a) for a in (w_t, r_t)),
    )(w_t, r_t)


def solution(mesh):
    feats = mesh.shape["feat"]

    def local_solve(design, targets, weights, step_sizes):
        w_t, r_t = solve(feats // CORES, design, weights.T, targets.T, step_sizes[None, :])
        w_t, r_t = trim(targets.shape[1], feats // CORES, w_t, r_t)
        return w_t.T, r_t.T

    return jax.shard_map(
        local_solve,
        mesh=mesh,
        in_specs=(P('prob', 'feat'), P('prob', None), P(('prob', 'feat'), None), P(('prob', 'feat'))),
        out_specs=(P(('prob', 'feat'), None), P('prob', None)),
        check_vma=False,
    )
```

```python
import functools

import jax
import jax.numpy as jnp
from jax import lax
from jax.experimental import pallas as pl
from jax.experimental.pallas import tpu as pltpu
from jax.sharding import PartitionSpec as P

SWEEPS = 6
RIDGE_COEF = 1.0
MIX_WEIGHT = 0.75
CORES = 2
ROW_TILE = 16
PIECES = 5
TURN = 32
RUNS = (7, 6, 4, 1, 1, 1, 1, 1, 1, 2, 3, 2, 2, 1, 2, 3, 4, 3, 2, 4, 2, 1, 3, 2,
        1, 5, 4, 1, 1, 3, 2, 2, 3, 1, 1, 2, 1, 5, 4, 1, 2, 5, 5, 1, 1, 4)
MESH = pl.DeviceIdType.MESH


def split_rows(padded):
    first = -(-padded // (2 * ROW_TILE)) * ROW_TILE
    return ((0, first), (first, padded - first))


def split_pieces(rows):
    size = -(-rows // (PIECES * ROW_TILE)) * ROW_TILE
    return tuple((r, min(size, rows - r)) for r in range(0, rows, size))


def sweep_steps(far, pieces):
    steps = []
    for t in range(1, far + 1):
        steps += [("send", t, p) for p in pieces]
        v = far - t
        steps += [("product", u, 0) for u in ((v, -v) if v else (0,))]
    steps += [("finish", 0, p) for p in pieces]
    for t in range(1, far + 1):
        steps += [("gather", t, p) for p in pieces]
        steps += [("gradient", t - 1, 0)]
    return steps + [("update", 0, 0)]


def schedule(group, far):
    lists = []
    for h, s in enumerate(group):
        steps = [(s,) + step for step in sweep_steps(far, s.pieces)]
        turn = TURN if h else len(steps)
        lists.append([step + (1,) for step in steps[turn:]] + [step + (0,) for step in steps[:turn]])
    order, h = [], 0
    for run in RUNS:
        order += lists[h][:run]
        del lists[h][:run]
        h = 1 - h
    return order + lists[0] + lists[1]


def kernel(chips, samples, streams, x_hbm, w_hbm, y_hbm, eta_ref, wout_hbm, rout_hbm,
           x, wraw, yraw, w, res, grad, op, xsem, wsem, ysem, *rest):
    per = len(rest) // len(streams)
    st = [rest[i * per:(i + 1) * per] for i in range(len(streams))]
    far, near = chips // 2, chips - 1 - chips // 2
    block = samples // (chips * CORES)
    rows_chip = block * CORES
    depth = x.shape[1]
    ridge_val = RIDGE_COEF / samples

    prob = lax.axis_index("prob")
    feat = lax.axis_index("feat")
    z, c = feat // CORES, feat % CORES
    other = 1 - c
    sgn = 1 - 2 * c

    def chip_at(v):
        return lax.rem(z + v * sgn + chips, chips)

    sib = (prob, z * CORES + other)
    nbr_p = (prob, chip_at(1) * CORES + c)
    nbr_q = (prob, chip_at(-1) * CORES + c)

    def x_rows(v):
        return pl.ds(pl.multiple_of(chip_at(v) * rows_chip, rows_chip), rows_chip)

    def remote(src, dst, ssem, rsem, dev):
        return pltpu.make_async_remote_copy(src_ref=src, dst_ref=dst, send_sem=ssem, recv_sem=rsem,
                                            device_id=dev, device_id_type=MESH)

    def x_copy(v):
        return pltpu.make_async_copy(x_hbm.at[x_rows(v), :], x.at[x_rows(v), :], xsem.at[v % chips])

    class Stream:
        def __init__(self, index):
            self.r0, self.rows = streams[index]
            self.rs = pl.ds(self.r0, self.rows)
            self.cuts = split_pieces(self.rows)
            self.pieces = range(len(self.cuts))
            (self.pbuf, self.precv, self.rp, self.rq, self.rbf, self.rfin,
             self.pd_s, self.pd_r, self.rsp_s, self.rsp_r, self.rsq_s, self.rsq_r,
             self.agp_s, self.agp_r, self.agq_s, self.agq_r, self.agd_s, self.agd_r, self.osem, self.wosem) = st[index]

        def ps(self, p):
            return pl.ds(*self.cuts[p])

        def pd(self, v):
            a, b = v % chips, -v % chips
            return remote(self.pbuf.at[a, other], self.precv.at[b], self.pd_s.at[a], self.pd_r.at[b], sib)

        def rs_p(self, t, p):
            ps = self.ps(p)
            return remote(self.pbuf.at[far + 1 - t, c, ps], self.rp.at[t - 1, ps], self.rsp_s.at[t - 1, p],
                          self.rsp_r.at[t - 1, p], nbr_p)

        def rs_q(self, t, p):
            ps = self.ps(p)
            return remote(self.pbuf.at[-(near + 1 - t) % chips, c, ps], self.rq.at[t - 1, ps],
                          self.rsq_s.at[t - 1, p], self.rsq_r.at[t - 1, p], nbr_q)

        def ag_p(self, buf, t, p):
            ps = self.ps(p)
            return remote(buf.at[t - 1, c, ps], buf.at[t, c, ps], self.agp_s.at[t - 1, p],
                          self.agp_r.at[t - 1, p], nbr_p)

        def ag_q(self, buf, t, p):
            ps = self.ps(p)
            return remote(buf.at[-(t - 1) % chips, c, ps], buf.at[-t % chips, c, ps], self.agq_s.at[t - 1, p],
                          self.agq_r.at[t - 1, p], nbr_q)

        def ag_d(self, buf, u, p):
            a, b, ps = u % chips, -u % chips, self.ps(p)
            return remote(buf.at[a, c, ps], buf.at[b, c, ps], self.agd_s.at[a, p], self.agd_r.at[b, p], sib)

        def ag_d_in(self, buf, u, p):
            a, ps = u % chips, self.ps(p)
            return remote(buf.at[a, other, ps], buf.at[a, other, ps], self.agd_s.at[a, p], self.agd_r.at[a, p], sib)

        def product(self, v):
            out = lax.dot_general(op[self.rs, :], x[x_rows(v), :], (((1,), (1,)), ((), ())),
                                  preferred_element_type=jnp.float32)
            for core in range(CORES):
                self.pbuf[v % chips, core] = out[:, core * block:(core + 1) * block]
            self.pd(v).start()

        def pass_on(self, t, p):
            ps = self.ps(p)
            v = far + 1 - t
            if p == 0:
                self.pd(-v).wait_recv()
            total = self.pbuf[v, c, ps] + self.precv[v, ps]
            if t > 1:
                self.rs_p(t - 1, p).wait_recv()
                total = total + self.rp[t - 2, ps]
            self.pbuf[v, c, ps] = total
            self.rs_p(t, p).start()
            t = t - 1
            if t >= 1:
                v = near + 1 - t
                slot = -v % chips
                if p == 0:
                    self.pd(v).wait_recv()
                total = self.pbuf[slot, c, ps] + self.precv[slot, ps]
                if t > 1:
                    self.rs_q(t - 1, p).wait_recv()
                    total = total + self.rq[t - 2, ps]
                self.pbuf[slot, c, ps] = total
                self.rs_q(t, p).start()

        def finish(self, it, p):
            ps = self.ps(p)
            if p == 0:
                self.pd(0).wait_recv()
            total = self.pbuf[0, c, ps] + self.precv[0, ps]
            self.rs_p(far, p).wait_recv()
            self.rs_q(near, p).wait_recv()
            total = total + self.rp[far - 1, ps] + self.rq[near - 1, ps]
            coef = jnp.where(it == 0, 1.0, MIX_WEIGHT).astype(jnp.float32)
            start, size = self.cuts[p]
            rs = pl.ds(self.r0 + start, size)
            new = res[rs, :] - coef * total
            res[rs, :] = new

            @pl.when(it < SWEEPS)
            def _():
                self.rbf[0, c, ps] = new.astype(jnp.bfloat16)
                self.ag_open(self.rbf, p)

            @pl.when(it == SWEEPS)
            def _():
                self.rfin[0, c, ps] = new
                self.ag_open(self.rfin, p)

        def ag_open(self, buf, p):
            self.ag_p(buf, 1, p).start()
            self.ag_q(buf, 1, p).start()
            self.ag_d(buf, 0, p).start()

        def ag_step(self, buf, t, p):
            self.ag_p(buf, t, p).wait_recv()
            if t < far:
                self.ag_p(buf, t + 1, p).start()
            self.ag_d(buf, t, p).start()
            if t <= near:
                self.ag_q(buf, t, p).wait_recv()
                if t < near:
                    self.ag_q(buf, t + 1, p).start()
                self.ag_d(buf, -t, p).start()

        def settle_sums(self):
            for v in range(chips):
                self.pd(v).wait_send()
            for p in self.pieces:
                for t in range(1, far + 1):
                    self.rs_p(t, p).wait_send()
                for t in range(1, near + 1):
                    self.rs_q(t, p).wait_send()

        def settle_gather(self, buf):
            for p in self.pieces:
                for t in range(1, far + 1):
                    self.ag_p(buf, t, p).wait_send()
                for t in range(1, near + 1):
                    self.ag_q(buf, t, p).wait_send()
                for u in range(chips):
                    self.ag_d(buf, u, p).wait_send()

        def gradient(self, t):
            offsets = (t, -t) if 0 < t <= near else (t,)
            parts = []
            for u in offsets:
                for p in self.pieces:
                    self.ag_d_in(self.rbf, u, p).wait_recv()
                parts.append((jnp.concatenate([self.rbf[u % chips, core] for core in range(CORES)], axis=1), x_rows(-u)))
            wide = min(depth, 1024)
            for j in range(depth // wide):
                cols = pl.ds(j * wide, wide)
                total = None if t == 0 else grad[self.rs, cols]
                for lhs, where in parts:
                    term = jnp.dot(lhs, x[where, cols], preferred_element_type=jnp.float32)
                    total = term if total is None else total + term
                grad[self.rs, cols] = total

        def step(self):
            @pl.loop(0, self.rows // ROW_TILE)
            def _(i):
                rs = pl.ds(pl.multiple_of(self.r0 + i * ROW_TILE, ROW_TILE), ROW_TILE)
                old = w[rs, :]
                update = eta_ref[...] * (grad[rs, :] * (1.0 / samples) - ridge_val * old)
                w[rs, :] = old + MIX_WEIGHT * update
                op[rs, :] = update.astype(jnp.bfloat16)

        def cast(self):
            k = wraw.shape[0]
            real = min(self.rows, k - self.r0)

            def move(rs):
                rows = wraw[rs, :]
                w[rs, :] = rows
                op[rs, :] = rows.astype(jnp.bfloat16)

            @pl.loop(0, real // ROW_TILE)
            def _(i):
                move(pl.ds(pl.multiple_of(self.r0 + i * ROW_TILE, ROW_TILE), ROW_TILE))

            if real % ROW_TILE:
                move(pl.ds(self.r0 + real // ROW_TILE * ROW_TILE, real % ROW_TILE))

        def write_w(self):
            return pltpu.make_async_copy(w.at[self.rs, :], wout_hbm.at[self.rs, :], self.wosem)

        def write(self, u, core):
            return pltpu.make_async_copy(self.rfin.at[u % chips, core],
                                         rout_hbm.at[self.rs, pl.ds(pl.multiple_of((chip_at(-u) * CORES + core) * block, block), block)],
                                         self.osem.at[u % chips, core])

    group = [Stream(i) for i in range(len(streams))]
    order = [far] + [s * v for v in range(near, 0, -1) for s in (1, -1)] + [0]

    w_copy = pltpu.make_async_copy(w_hbm, wraw, wsem)
    w_copy.start()
    x_copy(far).start()
    for v in order[1:]:
        x_copy(v).start()
    mine = pl.ds(pl.multiple_of(feat * block, block), block)
    y_copy = pltpu.make_async_copy(y_hbm.at[:, mine], yraw, ysem)
    y_copy.start()

    barrier = pltpu.get_barrier_semaphore()
    for dev in (sib, nbr_p, nbr_q):
        pl.semaphore_signal(barrier, inc=1, device_id=dev, device_id_type=MESH)
    pl.semaphore_wait(barrier, 3)

    w_copy.wait()
    for s in group:
        s.cast()
    x_copy(far).wait()
    for s in group:
        s.product(far)
    y_copy.wait()
    res[pl.ds(0, yraw.shape[0]), :] = yraw[...]

    def write_in(s, u):
        for p in s.pieces:
            s.ag_d_in(s.rfin, u, p).wait_recv()
        s.write(u, other).start()

    def sum_step(s, kind, a, p, it, loads):
        if kind == "send":
            s.pass_on(a, p)
        elif kind == "finish":
            s.finish(it, p)
        else:
            if (s, a) in loads:
                @pl.when(it == 0)
                def _():
                    x_copy(a).wait()
            s.product(a)

    def gather_step(s, kind, a, p, it):
        if kind == "gather":
            s.ag_step(s.rbf, a, p)
        elif kind == "gradient":
            s.gradient(a)
        else:
            s.gradient(far)
            s.step()
            s.settle_sums()
            s.settle_gather(s.rbf)
            s.product(far)

            @pl.when(it == SWEEPS - 1)
            def _():
                s.write_w().start()

    def last_step(s, kind, a, p):
        if kind == "gather":
            s.ag_step(s.rfin, a, p)
        elif kind == "gradient":
            for u in ((0,) if a == 0 else (a, -a)):
                s.write(u, c).start()
                write_in(s, u)
        else:
            s.write(far, c).start()
            write_in(s, far)

    steps = schedule(group, far)
    lag = max(step[-1] for step in steps)
    loads, seen = set(), set()
    for j in range(lag + 1):
        for s, kind, a, _, stage in steps:
            if kind == "product" and j == stage and a not in seen:
                seen.add(a)
                loads.add((s, a))
    batches = []
    for step in steps:
        key = (step[1] in ("send", "product", "finish"), step[-1])
        if not batches or batches[-1][0] != key:
            batches.append((key, []))
        batches[-1][1].append(step[:-1])

    @pl.loop(0, SWEEPS + 1 + lag)
    def _(j):
        for (sums, stage), batch in batches:
            it = j - stage
            if sums:
                @pl.when((it >= 0) & (it <= SWEEPS))
                def _():
                    for step in batch:
                        sum_step(*step, it, loads)
            else:
                @pl.when((it >= 0) & (it < SWEEPS))
                def _():
                    for step in batch:
                        gather_step(*step, it)

                @pl.when(it == SWEEPS)
                def _():
                    for step in batch:
                        last_step(*step)

    for s in group:
        s.settle_sums()
        s.settle_gather(s.rfin)
        for u in range(chips):
            for core in (c, other):
                s.write(u, core).wait()
        s.write_w().wait()


def solve(chips, design, w_t, y_t, eta):
    samples, depth = design.shape
    padded = -(-w_t.shape[0] // ROW_TILE) * ROW_TILE
    block = samples // (chips * CORES)
    far, near = chips // 2, chips - 1 - chips // 2
    streams = split_rows(padded)
    dma = pltpu.SemaphoreType.DMA
    f32, bf16 = jnp.float32, jnp.bfloat16
    scratch = [
        pltpu.VMEM((samples, depth), bf16),
        pltpu.VMEM((w_t.shape[0], depth), f32),
        pltpu.VMEM((w_t.shape[0], block), f32),
        pltpu.VMEM((padded, depth), f32),
        pltpu.VMEM((padded, block), f32),
        pltpu.VMEM((padded, depth), f32),
        pltpu.VMEM((padded, depth), bf16),
        dma((chips,)), dma, dma,
    ]
    for _, rows in streams:
        scratch += [
            pltpu.VMEM((chips, CORES, rows, block), f32),
            pltpu.VMEM((chips, rows, block), f32),
            pltpu.VMEM((far, rows, block), f32),
            pltpu.VMEM((near, rows, block), f32),
            pltpu.VMEM((chips, CORES, rows, block), bf16),
            pltpu.VMEM((chips, CORES, rows, block), f32),
            dma((chips,)), dma((chips,)),
            *[dma((hops, PIECES)) for hops in (far, far, near, near) * 2],
            dma((chips, PIECES)), dma((chips, PIECES)),
            dma((chips, CORES)), dma,
        ]
    any_spec = pl.BlockSpec(memory_space=pl.ANY)
    return pl.pallas_call(
        functools.partial(kernel, chips, samples, streams),
        out_shape=(jax.ShapeDtypeStruct((padded, depth), f32),
                   jax.ShapeDtypeStruct((padded, samples), f32)),
        in_specs=[any_spec, any_spec, any_spec, pl.BlockSpec(memory_space=pltpu.VMEM)],
        out_specs=(any_spec, any_spec),
        scratch_shapes=scratch,
        compiler_params=pltpu.CompilerParams(collective_id=0, has_side_effects=True,
                                             vmem_limit_bytes=56 * 1024 * 1024),
    )(design, w_t, y_t, eta)


def trim_kernel(k, w_in, r_in, w_out, r_out):
    w_out[...] = w_in[:k, :]
    r_out[...] = r_in[:k, :]


def trim(k, steps, w_t, r_t):
    def spec(rows, arr):
        return pl.BlockSpec((rows, arr.shape[1] // steps), lambda i: (0, i))

    return pl.pallas_call(
        functools.partial(trim_kernel, k),
        out_shape=tuple(jax.ShapeDtypeStruct((k, a.shape[1]), a.dtype) for a in (w_t, r_t)),
        grid=(steps,),
        in_specs=[spec(a.shape[0], a) for a in (w_t, r_t)],
        out_specs=tuple(spec(k, a) for a in (w_t, r_t)),
    )(w_t, r_t)


def solution(mesh):
    feats = mesh.shape["feat"]

    def local_solve(design, targets, weights, step_sizes):
        w_t, r_t = solve(feats // CORES, design, weights.T, targets.T, step_sizes[None, :])
        w_t, r_t = trim(targets.shape[1], feats // CORES, w_t, r_t)
        return w_t.T, r_t.T

    return jax.shard_map(
        local_solve,
        mesh=mesh,
        in_specs=(P('prob', 'feat'), P('prob', None), P(('prob', 'feat'), None), P(('prob', 'feat'))),
        out_specs=(P(('prob', 'feat'), None), P('prob', None)),
        check_vma=False,
    )
```

```python
import functools

import jax
import jax.numpy as jnp
from jax import lax
from jax.experimental import pallas as pl
from jax.experimental.pallas import tpu as pltpu
from jax.sharding import PartitionSpec as P

SWEEPS = 6
RIDGE_COEF = 1.0
MIX_WEIGHT = 0.75
CORES = 2
ROW_TILE = 16
PIECES = 2
TILES = (7, 6, 6)
TURNS = (None, 26, 17)
RUNS = (
    (0, 4), (2, 2), (1, 1), (2, 1), (1, 2), (0, 2), (1, 1), (2, 1), (0, 2), (2, 1), (1, 3),
    (2, 1), (0, 1), (1, 1), (0, 1), (2, 1), (0, 2), (2, 2), (1, 2), (0, 1), (1, 2), (2, 1),
    (0, 2), (2, 2), (1, 1), (2, 1), (1, 3), (0, 1), (2, 1), (0, 1), (2, 3), (1, 3), (0, 2),
    (2, 3), (1, 2), (2, 1), (0, 3), (2, 2), (1, 1), (2, 2), (1, 1), (0, 3), (1, 1), (2, 1),
    (0, 1), (2, 2), (1, 1), (0, 1), (1, 1), (0, 1), (1, 1), (0, 1), (2, 1), (0, 1), (2, 1),
    (1, 3),
)
MESH = pl.DeviceIdType.MESH


def split_rows(padded):
    sizes = [tiles * ROW_TILE for tiles in TILES]
    assert sum(sizes) == padded
    return tuple((sum(sizes[:i]), size) for i, size in enumerate(sizes))


def split_pieces(rows):
    size = -(-rows // (PIECES * ROW_TILE)) * ROW_TILE
    return tuple((r, min(size, rows - r)) for r in range(0, rows, size))


def sweep_steps(far, pieces):
    steps = []
    for t in range(1, far + 1):
        steps += [("send", t, p) for p in pieces]
        v = far - t
        steps += [("product", u, 0) for u in ((v, -v) if v else (0,))]
    steps += [("finish", 0, p) for p in pieces]
    for t in range(1, far + 1):
        steps += [("gather", t, p) for p in pieces]
        steps += [("gradient", t - 1, 0)]
    return steps + [("update", 0, 0)]


def schedule(group, far):
    lists = []
    for h, s in enumerate(group):
        steps = [(s,) + step for step in sweep_steps(far, s.pieces)]
        turn = len(steps) if TURNS[h] is None else TURNS[h]
        lists.append([step + (1,) for step in steps[turn:]] + [step + (0,) for step in steps[:turn]])
    order = []
    for h, run in RUNS:
        order += lists[h][:run]
        del lists[h][:run]
    assert not any(lists)
    return order


def kernel(chips, samples, streams, x_hbm, w_hbm, y_hbm, eta_ref, wout_hbm, rout_hbm,
           x, wraw, yraw, w, res, grad, op, xsem, wsem, ysem, *rest):
    per = len(rest) // len(streams)
    st = [rest[i * per:(i + 1) * per] for i in range(len(streams))]
    far, near = chips // 2, chips - 1 - chips // 2
    block = samples // (chips * CORES)
    rows_chip = block * CORES
    depth = x.shape[1]
    ridge_val = RIDGE_COEF / samples

    prob = lax.axis_index("prob")
    feat = lax.axis_index("feat")
    z, c = feat // CORES, feat % CORES
    other = 1 - c
    sgn = 1 - 2 * c

    def chip_at(v):
        return lax.rem(z + v * sgn + chips, chips)

    sib = (prob, z * CORES + other)
    nbr_p = (prob, chip_at(1) * CORES + c)
    nbr_q = (prob, chip_at(-1) * CORES + c)

    def x_rows(v):
        return pl.ds(pl.multiple_of(chip_at(v) * rows_chip, rows_chip), rows_chip)

    def remote(src, dst, ssem, rsem, dev):
        return pltpu.make_async_remote_copy(src_ref=src, dst_ref=dst, send_sem=ssem, recv_sem=rsem,
                                            device_id=dev, device_id_type=MESH)

    def x_copy(v):
        return pltpu.make_async_copy(x_hbm.at[x_rows(v), :], x.at[x_rows(v), :], xsem.at[v % chips])

    class Stream:
        def __init__(self, index):
            self.r0, self.rows = streams[index]
            self.rs = pl.ds(self.r0, self.rows)
            self.cuts = split_pieces(self.rows)
            self.pieces = range(len(self.cuts))
            (self.pbuf, self.precv, self.rp, self.rq, self.rbf, self.rfin,
             self.pd_s, self.pd_r, self.rsp_s, self.rsp_r, self.rsq_s, self.rsq_r,
             self.agp_s, self.agp_r, self.agq_s, self.agq_r, self.agd_s, self.agd_r, self.osem, self.wosem) = st[index]

        def ps(self, p):
            return pl.ds(*self.cuts[p])

        def pd(self, v):
            a, b = v % chips, -v % chips
            return remote(self.pbuf.at[a, other], self.precv.at[b], self.pd_s.at[a], self.pd_r.at[b], sib)

        def rs_p(self, t, p):
            ps = self.ps(p)
            return remote(self.pbuf.at[far + 1 - t, c, ps], self.rp.at[t - 1, ps], self.rsp_s.at[t - 1, p],
                          self.rsp_r.at[t - 1, p], nbr_p)

        def rs_q(self, t, p):
            ps = self.ps(p)
            return remote(self.pbuf.at[-(near + 1 - t) % chips, c, ps], self.rq.at[t - 1, ps],
                          self.rsq_s.at[t - 1, p], self.rsq_r.at[t - 1, p], nbr_q)

        def ag_p(self, buf, t, p):
            ps = self.ps(p)
            return remote(buf.at[t - 1, c, ps], buf.at[t, c, ps], self.agp_s.at[t - 1, p],
                          self.agp_r.at[t - 1, p], nbr_p)

        def ag_q(self, buf, t, p):
            ps = self.ps(p)
            return remote(buf.at[-(t - 1) % chips, c, ps], buf.at[-t % chips, c, ps], self.agq_s.at[t - 1, p],
                          self.agq_r.at[t - 1, p], nbr_q)

        def ag_d(self, buf, u):
            a, b = u % chips, -u % chips
            return remote(buf.at[a, c], buf.at[b, c], self.agd_s.at[a], self.agd_r.at[b], sib)

        def ag_d_in(self, buf, u):
            a = u % chips
            return remote(buf.at[a, other], buf.at[a, other], self.agd_s.at[a], self.agd_r.at[a], sib)

        def product(self, v):
            out = lax.dot_general(op[self.rs, :], x[x_rows(v), :], (((1,), (1,)), ((), ())),
                                  preferred_element_type=jnp.float32)
            for core in range(CORES):
                self.pbuf[v % chips, core] = out[:, core * block:(core + 1) * block]
            self.pd(v).start()

        def pass_on(self, t, p):
            ps = self.ps(p)
            v = far + 1 - t
            if p == 0:
                self.pd(-v).wait_recv()
            total = self.pbuf[v, c, ps] + self.precv[v, ps]
            if t > 1:
                self.rs_p(t - 1, p).wait_recv()
                total = total + self.rp[t - 2, ps]
            self.pbuf[v, c, ps] = total
            self.rs_p(t, p).start()
            t = t - 1
            if t >= 1:
                v = near + 1 - t
                slot = -v % chips
                if p == 0:
                    self.pd(v).wait_recv()
                total = self.pbuf[slot, c, ps] + self.precv[slot, ps]
                if t > 1:
                    self.rs_q(t - 1, p).wait_recv()
                    total = total + self.rq[t - 2, ps]
                self.pbuf[slot, c, ps] = total
                self.rs_q(t, p).start()

        def finish(self, it, p):
            ps = self.ps(p)
            if p == 0:
                self.pd(0).wait_recv()
            total = self.pbuf[0, c, ps] + self.precv[0, ps]
            self.rs_p(far, p).wait_recv()
            self.rs_q(near, p).wait_recv()
            total = total + self.rp[far - 1, ps] + self.rq[near - 1, ps]
            coef = jnp.where(it == 0, 1.0, MIX_WEIGHT).astype(jnp.float32)
            start, size = self.cuts[p]
            rs = pl.ds(self.r0 + start, size)
            new = res[rs, :] - coef * total
            res[rs, :] = new

            @pl.when(it < SWEEPS)
            def _():
                self.rbf[0, c, ps] = new.astype(jnp.bfloat16)
                self.ag_open(self.rbf, p)

            @pl.when(it == SWEEPS)
            def _():
                self.rfin[0, c, ps] = new
                self.ag_open(self.rfin, p)

        def ag_open(self, buf, p):
            self.ag_p(buf, 1, p).start()
            self.ag_q(buf, 1, p).start()
            if p == self.pieces[-1]:
                self.ag_d(buf, 0).start()

        def ag_step(self, buf, t, p):
            self.ag_p(buf, t, p).wait_recv()
            if t < far:
                self.ag_p(buf, t + 1, p).start()
            if p == self.pieces[-1]:
                self.ag_d(buf, t).start()
            if t <= near:
                self.ag_q(buf, t, p).wait_recv()
                if t < near:
                    self.ag_q(buf, t + 1, p).start()
                if p == self.pieces[-1]:
                    self.ag_d(buf, -t).start()

        def settle_sums(self):
            for v in range(chips):
                self.pd(v).wait_send()
            for p in self.pieces:
                for t in range(1, far + 1):
                    self.rs_p(t, p).wait_send()
                for t in range(1, near + 1):
                    self.rs_q(t, p).wait_send()

        def settle_gather(self, buf):
            for p in self.pieces:
                for t in range(1, far + 1):
                    self.ag_p(buf, t, p).wait_send()
                for t in range(1, near + 1):
                    self.ag_q(buf, t, p).wait_send()
            for u in range(chips):
                self.ag_d(buf, u).wait_send()

        def gradient(self, t):
            offsets = (t, -t) if 0 < t <= near else (t,)
            parts = []
            for u in offsets:
                self.ag_d_in(self.rbf, u).wait_recv()
                parts.append((jnp.concatenate([self.rbf[u % chips, core] for core in range(CORES)], axis=1), x_rows(-u)))
            wide = min(depth, 1024)
            for j in range(depth // wide):
                cols = pl.ds(j * wide, wide)
                total = None if t == 0 else grad[self.rs, cols]
                for lhs, where in parts:
                    term = jnp.dot(lhs, x[where, cols], preferred_element_type=jnp.float32)
                    total = term if total is None else total + term
                grad[self.rs, cols] = total

        def step(self):
            @pl.loop(0, self.rows // ROW_TILE)
            def _(i):
                rs = pl.ds(pl.multiple_of(self.r0 + i * ROW_TILE, ROW_TILE), ROW_TILE)
                old = w[rs, :]
                update = eta_ref[...] * (grad[rs, :] * (1.0 / samples) - ridge_val * old)
                w[rs, :] = old + MIX_WEIGHT * update
                op[rs, :] = update.astype(jnp.bfloat16)

        def cast(self):
            k = wraw.shape[0]
            real = min(self.rows, k - self.r0)

            def move(rs):
                rows = wraw[rs, :]
                w[rs, :] = rows
                op[rs, :] = rows.astype(jnp.bfloat16)

            @pl.loop(0, real // ROW_TILE)
            def _(i):
                move(pl.ds(pl.multiple_of(self.r0 + i * ROW_TILE, ROW_TILE), ROW_TILE))

            if real % ROW_TILE:
                move(pl.ds(self.r0 + real // ROW_TILE * ROW_TILE, real % ROW_TILE))

        def write_w(self):
            return pltpu.make_async_copy(w.at[self.rs, :], wout_hbm.at[self.rs, :], self.wosem)

        def write(self, u, core):
            return pltpu.make_async_copy(self.rfin.at[u % chips, core],
                                         rout_hbm.at[self.rs, pl.ds(pl.multiple_of((chip_at(-u) * CORES + core) * block, block), block)],
                                         self.osem.at[u % chips, core])

    group = [Stream(i) for i in range(len(streams))]
    order = [far] + [s * v for v in range(near, 0, -1) for s in (1, -1)] + [0]

    w_copy = pltpu.make_async_copy(w_hbm, wraw, wsem)
    w_copy.start()
    x_copy(far).start()
    for v in order[1:]:
        x_copy(v).start()
    mine = pl.ds(pl.multiple_of(feat * block, block), block)
    y_copy = pltpu.make_async_copy(y_hbm.at[:, mine], yraw, ysem)
    y_copy.start()

    barrier = pltpu.get_barrier_semaphore()
    for dev in (sib, nbr_p, nbr_q):
        pl.semaphore_signal(barrier, inc=1, device_id=dev, device_id_type=MESH)
    pl.semaphore_wait(barrier, 3)

    w_copy.wait()
    for s in group:
        s.cast()
    x_copy(far).wait()
    for s in group:
        s.product(far)
    y_copy.wait()
    res[pl.ds(0, yraw.shape[0]), :] = yraw[...]

    def write_in(s, u):
        s.ag_d_in(s.rfin, u).wait_recv()
        s.write(u, other).start()

    def sum_step(s, kind, a, p, it, loads):
        if kind == "send":
            s.pass_on(a, p)
        elif kind == "finish":
            s.finish(it, p)
        else:
            if (s, a) in loads:
                @pl.when(it == 0)
                def _():
                    x_copy(a).wait()
            s.product(a)

    def gather_step(s, kind, a, p, it):
        if kind == "gather":
            s.ag_step(s.rbf, a, p)
        elif kind == "gradient":
            s.gradient(a)
        else:
            s.gradient(far)
            s.step()
            s.settle_sums()
            s.settle_gather(s.rbf)
            s.product(far)

            @pl.when(it == SWEEPS - 1)
            def _():
                s.write_w().start()

    def last_step(s, kind, a, p):
        if kind == "gather":
            s.ag_step(s.rfin, a, p)
        elif kind == "gradient":
            for u in ((0,) if a == 0 else (a, -a)):
                s.write(u, c).start()
                write_in(s, u)
        else:
            s.write(far, c).start()
            write_in(s, far)

    steps = schedule(group, far)
    lag = max(step[-1] for step in steps)
    loads, seen = set(), set()
    for j in range(lag + 1):
        for s, kind, a, _, stage in steps:
            if kind == "product" and j == stage and a not in seen:
                seen.add(a)
                loads.add((s, a))
    batches = []
    for step in steps:
        key = (step[1] in ("send", "product", "finish"), step[-1])
        if not batches or batches[-1][0] != key:
            batches.append((key, []))
        batches[-1][1].append(step[:-1])

    @pl.loop(0, SWEEPS + 1 + lag)
    def _(j):
        for (sums, stage), batch in batches:
            it = j - stage
            if sums:
                @pl.when((it >= 0) & (it <= SWEEPS))
                def _():
                    for step in batch:
                        sum_step(*step, it, loads)
            else:
                @pl.when((it >= 0) & (it < SWEEPS))
                def _():
                    for step in batch:
                        gather_step(*step, it)

                @pl.when(it == SWEEPS)
                def _():
                    for step in batch:
                        last_step(*step)

    for s in group:
        s.settle_sums()
        s.settle_gather(s.rfin)
        for u in range(chips):
            for core in (c, other):
                s.write(u, core).wait()
        s.write_w().wait()


def solve(chips, design, w_t, y_t, eta):
    samples, depth = design.shape
    padded = -(-w_t.shape[0] // ROW_TILE) * ROW_TILE
    block = samples // (chips * CORES)
    far, near = chips // 2, chips - 1 - chips // 2
    streams = split_rows(padded)
    dma = pltpu.SemaphoreType.DMA
    f32, bf16 = jnp.float32, jnp.bfloat16
    scratch = [
        pltpu.VMEM((samples, depth), bf16),
        pltpu.VMEM((w_t.shape[0], depth), f32),
        pltpu.VMEM((w_t.shape[0], block), f32),
        pltpu.VMEM((padded, depth), f32),
        pltpu.VMEM((padded, block), f32),
        pltpu.VMEM((padded, depth), f32),
        pltpu.VMEM((padded, depth), bf16),
        dma((chips,)), dma, dma,
    ]
    for _, rows in streams:
        scratch += [
            pltpu.VMEM((chips, CORES, rows, block), f32),
            pltpu.VMEM((chips, rows, block), f32),
            pltpu.VMEM((far, rows, block), f32),
            pltpu.VMEM((near, rows, block), f32),
            pltpu.VMEM((chips, CORES, rows, block), bf16),
            pltpu.VMEM((chips, CORES, rows, block), f32),
            dma((chips,)), dma((chips,)),
            *[dma((hops, PIECES)) for hops in (far, far, near, near) * 2],
            dma((chips,)), dma((chips,)),
            dma((chips, CORES)), dma,
        ]
    any_spec = pl.BlockSpec(memory_space=pl.ANY)
    return pl.pallas_call(
        functools.partial(kernel, chips, samples, streams),
        out_shape=(jax.ShapeDtypeStruct((padded, depth), f32),
                   jax.ShapeDtypeStruct((padded, samples), f32)),
        in_specs=[any_spec, any_spec, any_spec, pl.BlockSpec(memory_space=pltpu.VMEM)],
        out_specs=(any_spec, any_spec),
        scratch_shapes=scratch,
        compiler_params=pltpu.CompilerParams(collective_id=0, has_side_effects=True,
                                             vmem_limit_bytes=56 * 1024 * 1024),
    )(design, w_t, y_t, eta)


def trim_kernel(steps, w_in, r_in, w_out, r_out, w_a, w_b, r_a, r_b, isem, osem):
    arrays = ((w_in, w_a, w_b, w_out), (r_in, r_a, r_b, r_out))

    def fetch(n, i):
        src, a, _, _ = arrays[n]
        return pltpu.make_async_copy(src.at[:, pl.ds(i * a.shape[2], a.shape[2])], a.at[i], isem.at[n, i])

    def store(n, i):
        _, _, b, dst = arrays[n]
        return pltpu.make_async_copy(b.at[i], dst.at[:, pl.ds(i * b.shape[2], b.shape[2])], osem.at[n, i])

    every = [(n, i) for i in range(steps) for n in range(len(arrays))]
    for n, i in every:
        fetch(n, i).start()
    for n, i in every:
        fetch(n, i).wait()
        _, a, b, _ = arrays[n]
        b[i] = a[i, :b.shape[1], :]
        store(n, i).start()
    for n, i in every:
        store(n, i).wait()


def trim(k, steps, w_t, r_t):
    any_spec = pl.BlockSpec(memory_space=pltpu.HBM)
    arrays = (w_t, r_t)
    return pl.pallas_call(
        functools.partial(trim_kernel, steps),
        out_shape=tuple(jax.ShapeDtypeStruct((k, a.shape[1]), a.dtype) for a in arrays),
        in_specs=[any_spec, any_spec],
        out_specs=(any_spec, any_spec),
        scratch_shapes=[
            *[pltpu.VMEM((steps, rows, a.shape[1] // steps), a.dtype)
              for a in arrays for rows in (a.shape[0], k)],
            pltpu.SemaphoreType.DMA((2, steps)),
            pltpu.SemaphoreType.DMA((2, steps)),
        ],
        compiler_params=pltpu.CompilerParams(vmem_limit_bytes=60 * 1024 * 1024),
    )(w_t, r_t)


def solution(mesh):
    feats = mesh.shape["feat"]

    def local_solve(design, targets, weights, step_sizes):
        w_t, r_t = solve(feats // CORES, design, weights.T, targets.T, step_sizes[None, :])
        w_t, r_t = trim(targets.shape[1], feats // CORES, w_t, r_t)
        return w_t.T, r_t.T

    return jax.shard_map(
        local_solve,
        mesh=mesh,
        in_specs=(P('prob', 'feat'), P('prob', None), P(('prob', 'feat'), None), P(('prob', 'feat'))),
        out_specs=(P(('prob', 'feat'), None), P('prob', None)),
        check_vma=False,
    )
```

```python
import functools

import jax
import jax.numpy as jnp
from jax import lax
from jax.experimental import pallas as pl
from jax.experimental.pallas import tpu as pltpu
from jax.sharding import PartitionSpec as P

SWEEPS = 6
RIDGE_COEF = 1.0
MIX_WEIGHT = 0.75
CORES = 2
ROW_TILE = 16
PIECES = 3
TILES = (10, 9)
TURNS = (None, 22)
RUNS = (
    (0, 5), (1, 4), (0, 2), (1, 1), (0, 1), (1, 1), (0, 2), (1, 1), (0, 1), (1, 1), (0, 4),
    (1, 4), (0, 4), (1, 4), (0, 1), (1, 1), (0, 3), (1, 5), (0, 4), (1, 5), (0, 2), (1, 1),
    (0, 1), (1, 3), (0, 3), (1, 1), (0, 1), (1, 4), (0, 5), (1, 3),
)
MESH = pl.DeviceIdType.MESH


def split_rows(padded):
    sizes = [tiles * ROW_TILE for tiles in TILES]
    assert sum(sizes) == padded
    return tuple((sum(sizes[:i]), size) for i, size in enumerate(sizes))


def split_pieces(rows):
    size = -(-rows // (PIECES * ROW_TILE)) * ROW_TILE
    return tuple((r, min(size, rows - r)) for r in range(0, rows, size))


def sweep_steps(far, pieces):
    steps = []
    for t in range(1, far + 1):
        steps += [("send", t, p) for p in pieces]
        v = far - t
        steps += [("product", u, 0) for u in ((v, -v) if v else (0,))]
    steps += [("finish", 0, p) for p in pieces]
    for t in range(1, far + 1):
        steps += [("gather", t, p) for p in pieces]
        steps += [("gradient", t - 1, 0)]
    return steps + [("update", 0, 0)]


def schedule(group, far):
    lists = []
    for h, s in enumerate(group):
        steps = [(s,) + step for step in sweep_steps(far, s.pieces)]
        turn = len(steps) if TURNS[h] is None else TURNS[h]
        lists.append([step + (1,) for step in steps[turn:]] + [step + (0,) for step in steps[:turn]])
    order = []
    for h, run in RUNS:
        order += lists[h][:run]
        del lists[h][:run]
    assert not any(lists)
    return order


def kernel(chips, samples, streams, x_hbm, w_hbm, y_hbm, eta_ref, wout_hbm, rout_hbm,
           x, wraw, yraw, w, res, grad, op, xsem, wsem, ysem, *rest):
    per = len(rest) // len(streams)
    st = [rest[i * per:(i + 1) * per] for i in range(len(streams))]
    far, near = chips // 2, chips - 1 - chips // 2
    block = samples // (chips * CORES)
    rows_chip = block * CORES
    depth = x.shape[1]
    ridge_val = RIDGE_COEF / samples

    prob = lax.axis_index("prob")
    feat = lax.axis_index("feat")
    z, c = feat // CORES, feat % CORES
    other = 1 - c
    sgn = 1 - 2 * c

    def chip_at(v):
        return lax.rem(z + v * sgn + chips, chips)

    sib = (prob, z * CORES + other)
    nbr_p = (prob, chip_at(1) * CORES + c)
    nbr_q = (prob, chip_at(-1) * CORES + c)

    def x_rows(v):
        return pl.ds(pl.multiple_of(chip_at(v) * rows_chip, rows_chip), rows_chip)

    def remote(src, dst, ssem, rsem, dev):
        return pltpu.make_async_remote_copy(src_ref=src, dst_ref=dst, send_sem=ssem, recv_sem=rsem,
                                            device_id=dev, device_id_type=MESH)

    def x_copy(v):
        return pltpu.make_async_copy(x_hbm.at[x_rows(v), :], x.at[x_rows(v), :], xsem.at[v % chips])

    class Stream:
        def __init__(self, index):
            self.r0, self.rows = streams[index]
            self.rs = pl.ds(self.r0, self.rows)
            self.cuts = split_pieces(self.rows)
            self.pieces = range(len(self.cuts))
            (self.pbuf, self.precv, self.rp, self.rq, self.rbf, self.rfin,
             self.pd_s, self.pd_r, self.rsp_s, self.rsp_r, self.rsq_s, self.rsq_r,
             self.agp_s, self.agp_r, self.agq_s, self.agq_r, self.agd_s, self.agd_r, self.osem, self.wosem) = st[index]

        def ps(self, p):
            return pl.ds(*self.cuts[p])

        def pd(self, v):
            a, b = v % chips, -v % chips
            return remote(self.pbuf.at[a, other], self.precv.at[b], self.pd_s.at[a], self.pd_r.at[b], sib)

        def rs_p(self, t, p):
            ps = self.ps(p)
            return remote(self.pbuf.at[far + 1 - t, c, ps], self.rp.at[t - 1, ps], self.rsp_s.at[t - 1, p],
                          self.rsp_r.at[t - 1, p], nbr_p)

        def rs_q(self, t, p):
            ps = self.ps(p)
            return remote(self.pbuf.at[-(near + 1 - t) % chips, c, ps], self.rq.at[t - 1, ps],
                          self.rsq_s.at[t - 1, p], self.rsq_r.at[t - 1, p], nbr_q)

        def ag_p(self, buf, t, p):
            ps = self.ps(p)
            return remote(buf.at[t - 1, c, ps], buf.at[t, c, ps], self.agp_s.at[t - 1, p],
                          self.agp_r.at[t - 1, p], nbr_p)

        def ag_q(self, buf, t, p):
            ps = self.ps(p)
            return remote(buf.at[-(t - 1) % chips, c, ps], buf.at[-t % chips, c, ps], self.agq_s.at[t - 1, p],
                          self.agq_r.at[t - 1, p], nbr_q)

        def ag_d(self, buf, u):
            a, b = u % chips, -u % chips
            return remote(buf.at[a, c], buf.at[b, c], self.agd_s.at[a], self.agd_r.at[b], sib)

        def ag_d_in(self, buf, u):
            a = u % chips
            return remote(buf.at[a, other], buf.at[a, other], self.agd_s.at[a], self.agd_r.at[a], sib)

        def product(self, v):
            out = lax.dot_general(op[self.rs, :], x[x_rows(v), :], (((1,), (1,)), ((), ())),
                                  preferred_element_type=jnp.float32)
            for core in range(CORES):
                self.pbuf[v % chips, core] = out[:, core * block:(core + 1) * block]
            self.pd(v).start()

        def pass_on(self, t, p):
            ps = self.ps(p)
            v = far + 1 - t
            if p == 0:
                self.pd(-v).wait_recv()
            total = self.pbuf[v, c, ps] + self.precv[v, ps]
            if t > 1:
                self.rs_p(t - 1, p).wait_recv()
                total = total + self.rp[t - 2, ps]
            self.pbuf[v, c, ps] = total
            self.rs_p(t, p).start()
            t = t - 1
            if t >= 1:
                v = near + 1 - t
                slot = -v % chips
                if p == 0:
                    self.pd(v).wait_recv()
                total = self.pbuf[slot, c, ps] + self.precv[slot, ps]
                if t > 1:
                    self.rs_q(t - 1, p).wait_recv()
                    total = total + self.rq[t - 2, ps]
                self.pbuf[slot, c, ps] = total
                self.rs_q(t, p).start()

        def finish(self, it, p):
            ps = self.ps(p)
            if p == 0:
                self.pd(0).wait_recv()
            total = self.pbuf[0, c, ps] + self.precv[0, ps]
            self.rs_p(far, p).wait_recv()
            self.rs_q(near, p).wait_recv()
            total = total + self.rp[far - 1, ps] + self.rq[near - 1, ps]
            coef = jnp.where(it == 0, 1.0, MIX_WEIGHT).astype(jnp.float32)
            start, size = self.cuts[p]
            rs = pl.ds(self.r0 + start, size)
            new = res[rs, :] - coef * total
            res[rs, :] = new

            @pl.when(it < SWEEPS)
            def _():
                self.rbf[0, c, ps] = new.astype(jnp.bfloat16)
                self.ag_open(self.rbf, p)

            @pl.when(it == SWEEPS)
            def _():
                self.rfin[0, c, ps] = new
                self.ag_open(self.rfin, p)

        def ag_open(self, buf, p):
            self.ag_p(buf, 1, p).start()
            self.ag_q(buf, 1, p).start()
            if p == self.pieces[-1]:
                self.ag_d(buf, 0).start()

        def ag_step(self, buf, t, p):
            self.ag_p(buf, t, p).wait_recv()
            if t < far:
                self.ag_p(buf, t + 1, p).start()
            if p == self.pieces[-1]:
                self.ag_d(buf, t).start()
            if t <= near:
                self.ag_q(buf, t, p).wait_recv()
                if t < near:
                    self.ag_q(buf, t + 1, p).start()
                if p == self.pieces[-1]:
                    self.ag_d(buf, -t).start()

        def settle_sums(self):
            for v in range(chips):
                self.pd(v).wait_send()
            for p in self.pieces:
                for t in range(1, far + 1):
                    self.rs_p(t, p).wait_send()
                for t in range(1, near + 1):
                    self.rs_q(t, p).wait_send()

        def settle_gather(self, buf):
            for p in self.pieces:
                for t in range(1, far + 1):
                    self.ag_p(buf, t, p).wait_send()
                for t in range(1, near + 1):
                    self.ag_q(buf, t, p).wait_send()
            for u in range(chips):
                self.ag_d(buf, u).wait_send()

        def gradient(self, t):
            offsets = (t, -t) if 0 < t <= near else (t,)
            parts = []
            for u in offsets:
                self.ag_d_in(self.rbf, u).wait_recv()
                parts.append((jnp.concatenate([self.rbf[u % chips, core] for core in range(CORES)], axis=1), x_rows(-u)))
            wide = min(depth, 1024)
            for j in range(depth // wide):
                cols = pl.ds(j * wide, wide)
                total = None if t == 0 else grad[self.rs, cols]
                for lhs, where in parts:
                    term = jnp.dot(lhs, x[where, cols], preferred_element_type=jnp.float32)
                    total = term if total is None else total + term
                grad[self.rs, cols] = total

        def step(self):
            @pl.loop(0, self.rows // ROW_TILE)
            def _(i):
                rs = pl.ds(pl.multiple_of(self.r0 + i * ROW_TILE, ROW_TILE), ROW_TILE)
                old = w[rs, :]
                update = eta_ref[...] * (grad[rs, :] * (1.0 / samples) - ridge_val * old)
                w[rs, :] = old + MIX_WEIGHT * update
                op[rs, :] = update.astype(jnp.bfloat16)

        def cast(self):
            k = wraw.shape[0]
            real = min(self.rows, k - self.r0)

            def move(rs):
                rows = wraw[rs, :]
                w[rs, :] = rows
                op[rs, :] = rows.astype(jnp.bfloat16)

            @pl.loop(0, real // ROW_TILE)
            def _(i):
                move(pl.ds(pl.multiple_of(self.r0 + i * ROW_TILE, ROW_TILE), ROW_TILE))

            if real % ROW_TILE:
                move(pl.ds(self.r0 + real // ROW_TILE * ROW_TILE, real % ROW_TILE))

        def write_w(self):
            return pltpu.make_async_copy(w.at[self.rs, :], wout_hbm.at[self.rs, :], self.wosem)

        def write(self, u, core):
            return pltpu.make_async_copy(self.rfin.at[u % chips, core],
                                         rout_hbm.at[self.rs, pl.ds(pl.multiple_of((chip_at(-u) * CORES + core) * block, block), block)],
                                         self.osem.at[u % chips, core])

    group = [Stream(i) for i in range(len(streams))]
    order = [far] + [s * v for v in range(near, 0, -1) for s in (1, -1)] + [0]

    w_copy = pltpu.make_async_copy(w_hbm, wraw, wsem)
    w_copy.start()
    x_copy(far).start()
    mine = pl.ds(pl.multiple_of(feat * block, block), block)
    y_copy = pltpu.make_async_copy(y_hbm.at[:, mine], yraw, ysem)

    barrier = pltpu.get_barrier_semaphore()
    for dev in (sib, nbr_p, nbr_q):
        pl.semaphore_signal(barrier, inc=1, device_id=dev, device_id_type=MESH)

    w_copy.wait()
    for v in order[1:]:
        x_copy(v).start()
    y_copy.start()
    group[0].cast()
    x_copy(far).wait()
    pl.semaphore_wait(barrier, 3)
    group[0].product(far)
    for s in group[1:]:
        s.cast()
        s.product(far)
    y_copy.wait()
    res[pl.ds(0, yraw.shape[0]), :] = yraw[...]

    def write_in(s, u):
        s.ag_d_in(s.rfin, u).wait_recv()
        s.write(u, other).start()

    def sum_step(s, kind, a, p, it, loads):
        if kind == "send":
            s.pass_on(a, p)
        elif kind == "finish":
            s.finish(it, p)
        else:
            if (s, a) in loads:
                @pl.when(it == 0)
                def _():
                    x_copy(a).wait()
            s.product(a)

    def gather_step(s, kind, a, p, it):
        if kind == "gather":
            s.ag_step(s.rbf, a, p)
        elif kind == "gradient":
            s.gradient(a)
        else:
            s.gradient(far)
            s.step()
            s.settle_sums()
            s.settle_gather(s.rbf)
            s.product(far)

            @pl.when(it == SWEEPS - 1)
            def _():
                s.write_w().start()

    def last_step(s, kind, a, p):
        if kind == "gather":
            s.ag_step(s.rfin, a, p)
        elif kind == "gradient":
            for u in ((0,) if a == 0 else (a, -a)):
                s.write(u, c).start()
                write_in(s, u)
        else:
            s.write(far, c).start()
            write_in(s, far)

    steps = schedule(group, far)
    lag = max(step[-1] for step in steps)
    loads, seen = set(), set()
    for j in range(lag + 1):
        for s, kind, a, _, stage in steps:
            if kind == "product" and j == stage and a not in seen:
                seen.add(a)
                loads.add((s, a))
    batches = []
    for step in steps:
        key = (step[1] in ("send", "product", "finish"), step[-1])
        if not batches or batches[-1][0] != key:
            batches.append((key, []))
        batches[-1][1].append(step[:-1])

    @pl.loop(0, SWEEPS + 1 + lag)
    def _(j):
        for (sums, stage), batch in batches:
            it = j - stage
            if sums:
                @pl.when((it >= 0) & (it <= SWEEPS))
                def _():
                    for step in batch:
                        sum_step(*step, it, loads)
            else:
                @pl.when((it >= 0) & (it < SWEEPS))
                def _():
                    for step in batch:
                        gather_step(*step, it)

                @pl.when(it == SWEEPS)
                def _():
                    for step in batch:
                        last_step(*step)

    for s in group:
        s.settle_sums()
        s.settle_gather(s.rfin)
        for u in range(chips):
            for core in (c, other):
                s.write(u, core).wait()
        s.write_w().wait()


def solve(chips, design, w_t, y_t, eta):
    samples, depth = design.shape
    padded = -(-w_t.shape[0] // ROW_TILE) * ROW_TILE
    block = samples // (chips * CORES)
    far, near = chips // 2, chips - 1 - chips // 2
    streams = split_rows(padded)
    dma = pltpu.SemaphoreType.DMA
    f32, bf16 = jnp.float32, jnp.bfloat16
    scratch = [
        pltpu.VMEM((samples, depth), bf16),
        pltpu.VMEM((w_t.shape[0], depth), f32),
        pltpu.VMEM((w_t.shape[0], block), f32),
        pltpu.VMEM((padded, depth), f32),
        pltpu.VMEM((padded, block), f32),
        pltpu.VMEM((padded, depth), f32),
        pltpu.VMEM((padded, depth), bf16),
        dma((chips,)), dma, dma,
    ]
    for _, rows in streams:
        scratch += [
            pltpu.VMEM((chips, CORES, rows, block), f32),
            pltpu.VMEM((chips, rows, block), f32),
            pltpu.VMEM((far, rows, block), f32),
            pltpu.VMEM((near, rows, block), f32),
            pltpu.VMEM((chips, CORES, rows, block), bf16),
            pltpu.VMEM((chips, CORES, rows, block), f32),
            dma((chips,)), dma((chips,)),
            *[dma((hops, PIECES)) for hops in (far, far, near, near) * 2],
            dma((chips,)), dma((chips,)),
            dma((chips, CORES)), dma,
        ]
    any_spec = pl.BlockSpec(memory_space=pl.ANY)
    return pl.pallas_call(
        functools.partial(kernel, chips, samples, streams),
        out_shape=(jax.ShapeDtypeStruct((padded, depth), f32),
                   jax.ShapeDtypeStruct((padded, samples), f32)),
        in_specs=[any_spec, any_spec, any_spec, pl.BlockSpec(memory_space=pltpu.VMEM)],
        out_specs=(any_spec, any_spec),
        scratch_shapes=scratch,
        compiler_params=pltpu.CompilerParams(collective_id=0, has_side_effects=True,
                                             vmem_limit_bytes=56 * 1024 * 1024),
    )(design, w_t, y_t, eta)


def trim_kernel(steps, w_in, r_in, w_out, r_out, w_a, w_b, r_a, r_b, isem, osem):
    arrays = ((w_in, w_a, w_b, w_out), (r_in, r_a, r_b, r_out))

    def fetch(n, i):
        src, a, _, _ = arrays[n]
        return pltpu.make_async_copy(src.at[:, pl.ds(i * a.shape[2], a.shape[2])], a.at[i], isem.at[n, i])

    def store(n, i):
        _, _, b, dst = arrays[n]
        return pltpu.make_async_copy(b.at[i], dst.at[:, pl.ds(i * b.shape[2], b.shape[2])], osem.at[n, i])

    every = [(n, i) for i in range(steps) for n in range(len(arrays))]
    for n, i in every:
        fetch(n, i).start()
    for n, i in every:
        fetch(n, i).wait()
        _, a, b, _ = arrays[n]
        b[i] = a[i, :b.shape[1], :]
        store(n, i).start()
    for n, i in every:
        store(n, i).wait()


def trim(k, steps, w_t, r_t):
    any_spec = pl.BlockSpec(memory_space=pltpu.HBM)
    arrays = (w_t, r_t)
    return pl.pallas_call(
        functools.partial(trim_kernel, steps),
        out_shape=tuple(jax.ShapeDtypeStruct((k, a.shape[1]), a.dtype) for a in arrays),
        in_specs=[any_spec, any_spec],
        out_specs=(any_spec, any_spec),
        scratch_shapes=[
            *[pltpu.VMEM((steps, rows, a.shape[1] // steps), a.dtype)
              for a in arrays for rows in (a.shape[0], k)],
            pltpu.SemaphoreType.DMA((2, steps)),
            pltpu.SemaphoreType.DMA((2, steps)),
        ],
        compiler_params=pltpu.CompilerParams(vmem_limit_bytes=60 * 1024 * 1024),
    )(w_t, r_t)


def solution(mesh):
    feats = mesh.shape["feat"]

    def local_solve(design, targets, weights, step_sizes):
        w_t, r_t = solve(feats // CORES, design, weights.T, targets.T, step_sizes[None, :])
        w_t, r_t = trim(targets.shape[1], feats // CORES, w_t, r_t)
        return w_t.T, r_t.T

    return jax.shard_map(
        local_solve,
        mesh=mesh,
        in_specs=(P('prob', 'feat'), P('prob', None), P(('prob', 'feat'), None), P(('prob', 'feat'))),
        out_specs=(P(('prob', 'feat'), None), P('prob', None)),
        check_vma=False,
    )
```

```python
import functools

import jax
import jax.numpy as jnp
from jax import lax
from jax.experimental import pallas as pl
from jax.experimental.pallas import tpu as pltpu
from jax.sharding import PartitionSpec as P

SWEEPS = 6
RIDGE_COEF = 1.0
MIX_WEIGHT = 0.75
CORES = 2
ROW_TILE = 16
PIECES = 5
TURN = 32
RUNS = (7, 6, 4, 1, 1, 1, 1, 1, 1, 2, 3, 2, 2, 1, 2, 3, 4, 3, 2, 4, 2, 1, 3, 2,
        1, 5, 4, 1, 1, 3, 2, 2, 3, 1, 1, 2, 1, 5, 4, 1, 2, 5, 5, 1, 1, 4)
MESH = pl.DeviceIdType.MESH


def split_rows(padded):
    first = -(-padded // (2 * ROW_TILE)) * ROW_TILE
    return ((0, first), (first, padded - first))


def split_pieces(rows):
    size = -(-rows // (PIECES * ROW_TILE)) * ROW_TILE
    return tuple((r, min(size, rows - r)) for r in range(0, rows, size))


def sweep_steps(far, pieces):
    steps = []
    for t in range(1, far + 1):
        steps += [("send", t, p) for p in pieces]
        v = far - t
        steps += [("product", u, 0) for u in ((v, -v) if v else (0,))]
    steps += [("finish", 0, p) for p in pieces]
    for t in range(1, far + 1):
        steps += [("gather", t, p) for p in pieces]
        steps += [("gradient", t - 1, 0)]
    return steps + [("update", 0, 0)]


def schedule(group, far):
    lists = []
    for h, s in enumerate(group):
        steps = [(s,) + step for step in sweep_steps(far, s.pieces)]
        turn = TURN if h else len(steps)
        lists.append([step + (1,) for step in steps[turn:]] + [step + (0,) for step in steps[:turn]])
    order, h = [], 0
    for run in RUNS:
        order += lists[h][:run]
        del lists[h][:run]
        h = 1 - h
    return order + lists[0] + lists[1]


def kernel(chips, samples, streams, x_hbm, w_hbm, y_hbm, eta_ref, wout_hbm, rout_hbm,
           x, wraw, yraw, w, res, grad, op, xsem, wsem, ysem, *rest):
    per = len(rest) // len(streams)
    st = [rest[i * per:(i + 1) * per] for i in range(len(streams))]
    far, near = chips // 2, chips - 1 - chips // 2
    block = samples // (chips * CORES)
    rows_chip = block * CORES
    depth = x.shape[1]
    ridge_val = RIDGE_COEF / samples

    prob = lax.axis_index("prob")
    feat = lax.axis_index("feat")
    z, c = feat // CORES, feat % CORES
    other = 1 - c
    sgn = 1 - 2 * c

    def chip_at(v):
        return lax.rem(z + v * sgn + chips, chips)

    sib = (prob, z * CORES + other)
    nbr_p = (prob, chip_at(1) * CORES + c)
    nbr_q = (prob, chip_at(-1) * CORES + c)

    def x_rows(v):
        return pl.ds(pl.multiple_of(chip_at(v) * rows_chip, rows_chip), rows_chip)

    def remote(src, dst, ssem, rsem, dev):
        return pltpu.make_async_remote_copy(src_ref=src, dst_ref=dst, send_sem=ssem, recv_sem=rsem,
                                            device_id=dev, device_id_type=MESH)

    def x_copy(v):
        return pltpu.make_async_copy(x_hbm.at[x_rows(v), :], x.at[x_rows(v), :], xsem.at[v % chips])

    class Stream:
        def __init__(self, index):
            self.r0, self.rows = streams[index]
            self.rs = pl.ds(self.r0, self.rows)
            self.cuts = split_pieces(self.rows)
            self.pieces = range(len(self.cuts))
            (self.pbuf, self.precv, self.rp, self.rq, self.rbf, self.rfin,
             self.pd_s, self.pd_r, self.rsp_s, self.rsp_r, self.rsq_s, self.rsq_r,
             self.agp_s, self.agp_r, self.agq_s, self.agq_r, self.agd_s, self.agd_r, self.osem, self.wosem) = st[index]

        def ps(self, p):
            return pl.ds(*self.cuts[p])

        def pd(self, v):
            a, b = v % chips, -v % chips
            return remote(self.pbuf.at[a, other], self.precv.at[b], self.pd_s.at[a], self.pd_r.at[b], sib)

        def rs_p(self, t, p):
            ps = self.ps(p)
            return remote(self.pbuf.at[far + 1 - t, c, ps], self.rp.at[t - 1, ps], self.rsp_s.at[t - 1, p],
                          self.rsp_r.at[t - 1, p], nbr_p)

        def rs_q(self, t, p):
            ps = self.ps(p)
            return remote(self.pbuf.at[-(near + 1 - t) % chips, c, ps], self.rq.at[t - 1, ps],
                          self.rsq_s.at[t - 1, p], self.rsq_r.at[t - 1, p], nbr_q)

        def ag_p(self, buf, t, p):
            ps = self.ps(p)
            return remote(buf.at[t - 1, c, ps], buf.at[t, c, ps], self.agp_s.at[t - 1, p],
                          self.agp_r.at[t - 1, p], nbr_p)

        def ag_q(self, buf, t, p):
            ps = self.ps(p)
            return remote(buf.at[-(t - 1) % chips, c, ps], buf.at[-t % chips, c, ps], self.agq_s.at[t - 1, p],
                          self.agq_r.at[t - 1, p], nbr_q)

        def ag_d(self, buf, u, p):
            a, b, ps = u % chips, -u % chips, self.ps(p)
            return remote(buf.at[a, c, ps], buf.at[b, c, ps], self.agd_s.at[a, p], self.agd_r.at[b, p], sib)

        def ag_d_in(self, buf, u, p):
            a, ps = u % chips, self.ps(p)
            return remote(buf.at[a, other, ps], buf.at[a, other, ps], self.agd_s.at[a, p], self.agd_r.at[a, p], sib)

        def product(self, v):
            out = lax.dot_general(op[self.rs, :], x[x_rows(v), :], (((1,), (1,)), ((), ())),
                                  preferred_element_type=jnp.float32)
            for core in range(CORES):
                self.pbuf[v % chips, core] = out[:, core * block:(core + 1) * block]
            self.pd(v).start()

        def pass_on(self, t, p):
            ps = self.ps(p)
            v = far + 1 - t
            if p == 0:
                self.pd(-v).wait_recv()
            total = self.pbuf[v, c, ps] + self.precv[v, ps]
            if t > 1:
                self.rs_p(t - 1, p).wait_recv()
                total = total + self.rp[t - 2, ps]
            self.pbuf[v, c, ps] = total
            self.rs_p(t, p).start()
            t = t - 1
            if t >= 1:
                v = near + 1 - t
                slot = -v % chips
                if p == 0:
                    self.pd(v).wait_recv()
                total = self.pbuf[slot, c, ps] + self.precv[slot, ps]
                if t > 1:
                    self.rs_q(t - 1, p).wait_recv()
                    total = total + self.rq[t - 2, ps]
                self.pbuf[slot, c, ps] = total
                self.rs_q(t, p).start()

        def finish(self, it, p):
            ps = self.ps(p)
            if p == 0:
                self.pd(0).wait_recv()
            total = self.pbuf[0, c, ps] + self.precv[0, ps]
            self.rs_p(far, p).wait_recv()
            self.rs_q(near, p).wait_recv()
            total = total + self.rp[far - 1, ps] + self.rq[near - 1, ps]
            coef = jnp.where(it == 0, 1.0, MIX_WEIGHT).astype(jnp.float32)
            start, size = self.cuts[p]
            rs = pl.ds(self.r0 + start, size)
            new = res[rs, :] - coef * total
            res[rs, :] = new

            @pl.when(it < SWEEPS)
            def _():
                self.rbf[0, c, ps] = new.astype(jnp.bfloat16)
                self.ag_open(self.rbf, p)

            @pl.when(it == SWEEPS)
            def _():
                self.rfin[0, c, ps] = new
                self.ag_open(self.rfin, p)

        def ag_open(self, buf, p):
            self.ag_p(buf, 1, p).start()
            self.ag_q(buf, 1, p).start()
            self.ag_d(buf, 0, p).start()

        def ag_step(self, buf, t, p):
            self.ag_p(buf, t, p).wait_recv()
            if t < far:
                self.ag_p(buf, t + 1, p).start()
            self.ag_d(buf, t, p).start()
            if t <= near:
                self.ag_q(buf, t, p).wait_recv()
                if t < near:
                    self.ag_q(buf, t + 1, p).start()
                self.ag_d(buf, -t, p).start()

        def settle_sums(self):
            for v in range(chips):
                self.pd(v).wait_send()
            for p in self.pieces:
                for t in range(1, far + 1):
                    self.rs_p(t, p).wait_send()
                for t in range(1, near + 1):
                    self.rs_q(t, p).wait_send()

        def settle_gather(self, buf):
            for p in self.pieces:
                for t in range(1, far + 1):
                    self.ag_p(buf, t, p).wait_send()
                for t in range(1, near + 1):
                    self.ag_q(buf, t, p).wait_send()
                for u in range(chips):
                    self.ag_d(buf, u, p).wait_send()

        def gradient(self, t):
            offsets = (t, -t) if 0 < t <= near else (t,)
            parts = []
            for u in offsets:
                for p in self.pieces:
                    self.ag_d_in(self.rbf, u, p).wait_recv()
                parts.append((jnp.concatenate([self.rbf[u % chips, core] for core in range(CORES)], axis=1), x_rows(-u)))
            wide = min(depth, 1024)
            for j in range(depth // wide):
                cols = pl.ds(j * wide, wide)
                total = None if t == 0 else grad[self.rs, cols]
                for lhs, where in parts:
                    term = jnp.dot(lhs, x[where, cols], preferred_element_type=jnp.float32)
                    total = term if total is None else total + term
                grad[self.rs, cols] = total

        def step(self):
            @pl.loop(0, self.rows // ROW_TILE)
            def _(i):
                rs = pl.ds(pl.multiple_of(self.r0 + i * ROW_TILE, ROW_TILE), ROW_TILE)
                old = w[rs, :]
                update = eta_ref[...] * (grad[rs, :] * (1.0 / samples) - ridge_val * old)
                w[rs, :] = old + MIX_WEIGHT * update
                op[rs, :] = update.astype(jnp.bfloat16)

        def cast(self):
            k = wraw.shape[0]
            real = min(self.rows, k - self.r0)

            def move(rs):
                rows = wraw[rs, :]
                w[rs, :] = rows
                op[rs, :] = rows.astype(jnp.bfloat16)

            @pl.loop(0, real // ROW_TILE)
            def _(i):
                move(pl.ds(pl.multiple_of(self.r0 + i * ROW_TILE, ROW_TILE), ROW_TILE))

            if real % ROW_TILE:
                move(pl.ds(self.r0 + real // ROW_TILE * ROW_TILE, real % ROW_TILE))

        def write_w(self):
            return pltpu.make_async_copy(w.at[self.rs, :], wout_hbm.at[self.rs, :], self.wosem)

        def write(self, u, core):
            return pltpu.make_async_copy(self.rfin.at[u % chips, core],
                                         rout_hbm.at[self.rs, pl.ds(pl.multiple_of((chip_at(-u) * CORES + core) * block, block), block)],
                                         self.osem.at[u % chips, core])

    group = [Stream(i) for i in range(len(streams))]
    order = [far] + [s * v for v in range(near, 0, -1) for s in (1, -1)] + [0]

    w_copy = pltpu.make_async_copy(w_hbm, wraw, wsem)
    w_copy.start()
    x_copy(far).start()
    mine = pl.ds(pl.multiple_of(feat * block, block), block)
    y_copy = pltpu.make_async_copy(y_hbm.at[:, mine], yraw, ysem)

    barrier = pltpu.get_barrier_semaphore()
    for dev in (sib, nbr_p, nbr_q):
        pl.semaphore_signal(barrier, inc=1, device_id=dev, device_id_type=MESH)

    w_copy.wait()
    for v in order[1:]:
        x_copy(v).start()
    y_copy.start()
    group[0].cast()
    x_copy(far).wait()
    pl.semaphore_wait(barrier, 3)
    group[0].product(far)
    for s in group[1:]:
        s.cast()
        s.product(far)
    y_copy.wait()
    res[pl.ds(0, yraw.shape[0]), :] = yraw[...]

    def write_in(s, u):
        for p in s.pieces:
            s.ag_d_in(s.rfin, u, p).wait_recv()
        s.write(u, other).start()

    def sum_step(s, kind, a, p, it, loads):
        if kind == "send":
            s.pass_on(a, p)
        elif kind == "finish":
            s.finish(it, p)
        else:
            if (s, a) in loads:
                @pl.when(it == 0)
                def _():
                    x_copy(a).wait()
            s.product(a)

    def gather_step(s, kind, a, p, it):
        if kind == "gather":
            s.ag_step(s.rbf, a, p)
        elif kind == "gradient":
            s.gradient(a)
        else:
            s.gradient(far)
            s.step()
            s.settle_sums()
            s.settle_gather(s.rbf)
            s.product(far)

            @pl.when(it == SWEEPS - 1)
            def _():
                s.write_w().start()

    def last_step(s, kind, a, p):
        if kind == "gather":
            s.ag_step(s.rfin, a, p)
        elif kind == "gradient":
            for u in ((0,) if a == 0 else (a, -a)):
                s.write(u, c).start()
                write_in(s, u)
        else:
            s.write(far, c).start()
            write_in(s, far)

    steps = schedule(group, far)
    lag = max(step[-1] for step in steps)
    loads, seen = set(), set()
    for j in range(lag + 1):
        for s, kind, a, _, stage in steps:
            if kind == "product" and j == stage and a not in seen:
                seen.add(a)
                loads.add((s, a))
    batches = []
    for step in steps:
        key = (step[1] in ("send", "product", "finish"), step[-1])
        if not batches or batches[-1][0] != key:
            batches.append((key, []))
        batches[-1][1].append(step[:-1])

    @pl.loop(0, SWEEPS + 1 + lag)
    def _(j):
        for (sums, stage), batch in batches:
            it = j - stage
            if sums:
                @pl.when((it >= 0) & (it <= SWEEPS))
                def _():
                    for step in batch:
                        sum_step(*step, it, loads)
            else:
                @pl.when((it >= 0) & (it < SWEEPS))
                def _():
                    for step in batch:
                        gather_step(*step, it)

                @pl.when(it == SWEEPS)
                def _():
                    for step in batch:
                        last_step(*step)

    for s in group:
        s.settle_sums()
        s.settle_gather(s.rfin)
        for u in range(chips):
            for core in (c, other):
                s.write(u, core).wait()
        s.write_w().wait()


def solve(chips, design, w_t, y_t, eta):
    samples, depth = design.shape
    padded = -(-w_t.shape[0] // ROW_TILE) * ROW_TILE
    block = samples // (chips * CORES)
    far, near = chips // 2, chips - 1 - chips // 2
    streams = split_rows(padded)
    dma = pltpu.SemaphoreType.DMA
    f32, bf16 = jnp.float32, jnp.bfloat16
    scratch = [
        pltpu.VMEM((samples, depth), bf16),
        pltpu.VMEM((w_t.shape[0], depth), f32),
        pltpu.VMEM((w_t.shape[0], block), f32),
        pltpu.VMEM((padded, depth), f32),
        pltpu.VMEM((padded, block), f32),
        pltpu.VMEM((padded, depth), f32),
        pltpu.VMEM((padded, depth), bf16),
        dma((chips,)), dma, dma,
    ]
    for _, rows in streams:
        scratch += [
            pltpu.VMEM((chips, CORES, rows, block), f32),
            pltpu.VMEM((chips, rows, block), f32),
            pltpu.VMEM((far, rows, block), f32),
            pltpu.VMEM((near, rows, block), f32),
            pltpu.VMEM((chips, CORES, rows, block), bf16),
            pltpu.VMEM((chips, CORES, rows, block), f32),
            dma((chips,)), dma((chips,)),
            *[dma((hops, PIECES)) for hops in (far, far, near, near) * 2],
            dma((chips, PIECES)), dma((chips, PIECES)),
            dma((chips, CORES)), dma,
        ]
    any_spec = pl.BlockSpec(memory_space=pl.ANY)
    return pl.pallas_call(
        functools.partial(kernel, chips, samples, streams),
        out_shape=(jax.ShapeDtypeStruct((padded, depth), f32),
                   jax.ShapeDtypeStruct((padded, samples), f32)),
        in_specs=[any_spec, any_spec, any_spec, pl.BlockSpec(memory_space=pltpu.VMEM)],
        out_specs=(any_spec, any_spec),
        scratch_shapes=scratch,
        compiler_params=pltpu.CompilerParams(collective_id=0, has_side_effects=True,
                                             vmem_limit_bytes=56 * 1024 * 1024),
    )(design, w_t, y_t, eta)


def trim_kernel(steps, w_in, r_in, w_out, r_out, w_a, w_b, r_a, r_b, isem, osem):
    arrays = ((w_in, w_a, w_b, w_out), (r_in, r_a, r_b, r_out))

    def fetch(n, i):
        src, a, _, _ = arrays[n]
        return pltpu.make_async_copy(src.at[:, pl.ds(i * a.shape[2], a.shape[2])], a.at[i], isem.at[n, i])

    def store(n, i):
        _, _, b, dst = arrays[n]
        return pltpu.make_async_copy(b.at[i], dst.at[:, pl.ds(i * b.shape[2], b.shape[2])], osem.at[n, i])

    every = [(n, i) for i in range(steps) for n in range(len(arrays))]
    for n, i in every:
        fetch(n, i).start()
    for n, i in every:
        fetch(n, i).wait()
        _, a, b, _ = arrays[n]
        b[i] = a[i, :b.shape[1], :]
        store(n, i).start()
    for n, i in every:
        store(n, i).wait()


def trim(k, steps, w_t, r_t):
    any_spec = pl.BlockSpec(memory_space=pltpu.HBM)
    arrays = (w_t, r_t)
    return pl.pallas_call(
        functools.partial(trim_kernel, steps),
        out_shape=tuple(jax.ShapeDtypeStruct((k, a.shape[1]), a.dtype) for a in arrays),
        in_specs=[any_spec, any_spec],
        out_specs=(any_spec, any_spec),
        scratch_shapes=[
            *[pltpu.VMEM((steps, rows, a.shape[1] // steps), a.dtype)
              for a in arrays for rows in (a.shape[0], k)],
            pltpu.SemaphoreType.DMA((2, steps)),
            pltpu.SemaphoreType.DMA((2, steps)),
        ],
        compiler_params=pltpu.CompilerParams(vmem_limit_bytes=60 * 1024 * 1024),
    )(w_t, r_t)


def solution(mesh):
    feats = mesh.shape["feat"]

    def local_solve(design, targets, weights, step_sizes):
        w_t, r_t = solve(feats // CORES, design, weights.T, targets.T, step_sizes[None, :])
        w_t, r_t = trim(targets.shape[1], feats // CORES, w_t, r_t)
        return w_t.T, r_t.T

    return jax.shard_map(
        local_solve,
        mesh=mesh,
        in_specs=(P('prob', 'feat'), P('prob', None), P(('prob', 'feat'), None), P(('prob', 'feat'))),
        out_specs=(P(('prob', 'feat'), None), P('prob', None)),
        check_vma=False,
    )
```
